128 devices in a mesh: seq: 8 (over y_lo, x), tp: 8 (over z, core), grp: 2 (over y_hi).
Axes of the slice: x: 4, y: 4 (y_hi: 2, y_lo: 2; y = y_hi * 2 + y_lo), z: 4, core: 2. Of those that a mesh axis runs over, the one named last changes fastest.
Arguments:
- query: bfloat16 [16, 64, 8192], P('grp', None, 'tp'), parts along dimension 0, may hold values from -15 to 15
- cache: bfloat16 [16, 16384, 8, 256], P('grp', 'tp', 'seq'), parts along dimension 0, may hold values from -6 to 6
- head_of_slot: int32 [16], P('grp'), parts along dimension 0, may hold values from 0 to 7, each once
- lengths: int32 [16], P('grp'), parts along dimension 0, may hold values from 8192 to 16384
- out_weight: bfloat16 [8192, 8192], P('tp', 'seq'), may hold values from -0.0625 to 0.0625
Outputs:
- projected: bfloat16 [16, 64, 8192], P(('grp', 'tp'), None, 'seq'), parts along dimension 0
The draws below stay inside these ranges and needn't reach their ends.
There are 2 independent parts, one for each index of `grp`. The reference program is written for one: setup_inputs(seed, part) draws one part's arguments, and reference() takes and returns one part's arrays. A program takes and returns all parts, laid end to end along the dimension named above; an argument that names none is the same for every part. Nothing has to cross between parts.
Inputs may be any that keep to these rules, and one draw needn't show every extreme that they name: head_of_slot names every KV head exactly once.
All inputs are finite; a program needn't handle non-finite values.
Results may differ from the reference program's by a relative error of at most 0.01.
Values may be sent and summed in bfloat16 or wider, within the bound.
A program may use at most 128 MiB of HBM per device.

```python
import math
import jax
import jax.numpy as jnp
from jax import lax

D = 8192
HQ = 64
KVH = 8
HD = 128
B = 8
QT = 64
L = 16384


def draw_query(key, part):
    own_key = jax.random.fold_in(key, 11)
    values = jnp.clip(3.0 * jax.random.normal(own_key, (B, QT, HQ * HD), jnp.float32), -15.0, 15.0)
    return values.astype(jnp.bfloat16)


def draw_cache(key, part):
    own_key = jax.random.fold_in(key, 23)
    values = jnp.clip(jax.random.normal(own_key, (B, L, KVH, 2 * HD), jnp.float32), -6.0, 6.0)
    return values.astype(jnp.bfloat16)


def with_ends(values, key, smallest, top_value):
    shape = values.shape
    spot = [jax.random.randint(jax.random.fold_in(key, axis), (), 0, shape[axis]) for axis in range(len(shape))]
    values = values.at[tuple(spot)].set(smallest)
    longest = shape.index(max(shape))
    spot[longest] = (spot[longest] + 1) % shape[longest]
    return values.at[tuple(spot)].set(top_value)


def shard_levels(stream_key, extent, shards, smallest, top_value):
    factor_of = 1.0
    for position, parts in shards:
        heights = jax.random.uniform(jax.random.fold_in(jax.random.fold_in(stream_key, 6), position), (parts,), jnp.float32, smallest / len(shards), top_value / len(shards))
        factor_of = factor_of * jnp.repeat(jnp.exp(heights), extent[position] // parts).reshape((-1,) + (1,) * (len(extent) - 1 - position))
    return factor_of


def noise(key, shape, spread, bound, cuts=(), kind=jnp.bfloat16):
    loudness = shard_levels(key, shape, cuts, -0.22, 0.18) if cuts else 1.0
    drawn = jax.random.normal(key, shape, jnp.float32) * spread * loudness
    return jnp.minimum(jnp.maximum(drawn, -bound), bound).astype(kind)


def setup_inputs(seed: int = 0, part: int = 0) -> dict:
    arg_keys = jax.random.split(jax.random.key(seed), 6)
    own_keys = jax.random.split(jax.random.fold_in(arg_keys[5], part), 6)
    query = draw_query(jax.random.fold_in(jax.random.fold_in(arg_keys[5], part), 71), part)
    cache = draw_cache(jax.random.fold_in(jax.random.fold_in(arg_keys[5], part), 71), part)
    head_of_slot = jax.random.permutation(own_keys[2], KVH).astype(jnp.int32)
    lengths = with_ends(jax.random.randint(own_keys[3], (B,), L // 2, L + 1), jax.random.fold_in(own_keys[3], 1), L // 2, L).astype(jnp.int32)
    out_weight = noise(arg_keys[4], (HQ * HD, D), (HQ * HD) ** -0.5, 0.0625, ((0, 8), (1, 8)))
    return dict(query=query, cache=cache, head_of_slot=head_of_slot, lengths=lengths, out_weight=out_weight)


MASKED_SCORE = -1e+30

def reference(query, cache, head_of_slot, lengths, out_weight):
    group_size = HQ // KVH
    scaling = 1.0 / math.sqrt(HD)
    slot_ids = jnp.arange(KVH, dtype=jnp.int32)
    slot_of_head = lax.optimization_barrier(jnp.sum(jnp.where(head_of_slot[None, :] == slot_ids[:, None], slot_ids[None, :], 0), axis=1)).astype(jnp.int32)
    positions = jnp.arange(L, dtype=jnp.int32)
    row_token = jnp.arange(QT * group_size, dtype=jnp.int32) // group_size

    def attend_pair(pair_index):
        seq_index = pair_index // KVH
        kv_head = pair_index % KVH
        entries = lax.dynamic_index_in_dim(cache, seq_index, 0, False)
        entries = lax.dynamic_index_in_dim(entries, slot_of_head[kv_head], 1, False)
        queries = lax.dynamic_index_in_dim(query, seq_index, 0, False)
        queries = lax.dynamic_slice_in_dim(queries, kv_head * group_size * HD, group_size * HD, 1)
        queries = queries.reshape(QT * group_size, HD)
        scores = jnp.dot(queries, entries[:, :HD].T, preferred_element_type=jnp.float32) * scaling
        limits = lengths[seq_index] - QT + row_token
        visible = positions[None, :] <= limits[:, None]
        scores = jnp.where(visible, scores, MASKED_SCORE)
        maxima = lax.optimization_barrier(jnp.max(scores, axis=1))
        weights = jnp.where(visible, jnp.exp(scores - maxima[:, None]), 0.0)
        totals = lax.optimization_barrier(jnp.sum(weights, axis=1))
        blended = jnp.dot(weights.astype(jnp.bfloat16), entries[:, HD:], preferred_element_type=jnp.float32)
        return (blended / totals[:, None]).astype(jnp.bfloat16).reshape(QT, group_size * HD)
    attended = lax.map(attend_pair, jnp.arange(B * KVH, dtype=jnp.int32))
    attended = attended.reshape(B, KVH, QT, group_size * HD).transpose(0, 2, 1, 3).reshape(B * QT, HQ * HD)
    projected = jnp.dot(attended, out_weight, preferred_element_type=jnp.float32)
    return projected.astype(jnp.bfloat16).reshape(B, QT, D)
```

```python
import functools
import math

import jax
import jax.numpy as jnp
from jax import lax
from jax.experimental import pallas as pl
from jax.experimental.pallas import tpu as pltpu
from jax.sharding import PartitionSpec as P

HQ = 64
KVH = 8
HD = 128
NB = 8
QT = 64
GS = 8
ROWS = GS * QT
TILE = 256
MASKED = -1e30
EXP2_SCALE = math.log2(math.e) / math.sqrt(HD)
F32 = jnp.float32
BF16 = jnp.bfloat16
MESH = pl.DeviceIdType.MESH
Q0, Q1, Q2, Q3, ML, C1, C2, C3, C4 = range(9)
NCH = 4


def kernel(
    heads_ref, len_ref, q_hbm, kv_hbm, w_hbm, out_ref,
    qown, q0recv, cand, q1recv, qall, kv, w, kx, s0, s1, p0, p1, ms0, ms1,
    oacc, mlbuf, mlrecv, osend, c1recv, c2send, c2recv, psum, c3recv, attall,
    ybuf, d1recv, d2send, d2recv, ssem, rsem, dssem, drsem, lsem,
):
    s = lax.axis_index("seq")
    t = lax.axis_index("tp")
    z = t // 2
    c = t % 2
    other = 1 - c
    length = kv.shape[1]
    head = heads_ref[s]
    head_chip = head // 2
    head_core = head % 2

    def slot_of(h):
        slot = jnp.int32(0)
        for k in range(KVH):
            slot = jnp.where(heads_ref[k] == h, k, slot)
        return slot

    my_slots = [slot_of(2 * k + c) for k in range(4)]
    other_slots = [slot_of(2 * k + other) for k in range(4)]

    partner = {"tp": t + 1 - 2 * c}

    def zpeer(d):
        zz = (z + d) % 4
        return zz, {"tp": 2 * zz + c}

    def send(src, dst, ss, rs, dev):
        pltpu.make_async_remote_copy(
            src_ref=src, dst_ref=dst, send_sem=ss, recv_sem=rs, device_id=dev, device_id_type=MESH
        ).start()

    def got(ref, rs):
        pltpu.make_async_remote_copy(
            src_ref=ref, dst_ref=ref, send_sem=rs, recv_sem=rs, device_id=partner, device_id_type=MESH
        ).wait_recv()

    def sent(ref, ss):
        pltpu.make_async_remote_copy(
            src_ref=ref, dst_ref=ref, send_sem=ss, recv_sem=ss, device_id=partner, device_id_type=MESH
        ).wait_send()

    qload = pltpu.make_async_copy(q_hbm, qown, lsem.at[NB])
    qload.start()

    def kv_load(b):
        return pltpu.make_async_copy(kv_hbm.at[b], kv.at[b], lsem.at[b])

    wload = pltpu.make_async_copy(w_hbm, w, lsem.at[NB + 1])
    for b in range(NB):
        kv_load(b).start()
    wload.start()

    barrier = pltpu.get_barrier_semaphore()
    for d in range(1, 8):
        pl.semaphore_signal(barrier, inc=1, device_id={"tp": (t + d) % 8}, device_id_type=MESH)
        pl.semaphore_signal(barrier, inc=1, device_id={"seq": (s + d) % 8}, device_id_type=MESH)

    p1[...] = jnp.zeros_like(p1)
    qload.wait()
    pl.semaphore_wait(barrier, 14)

    half = pl.multiple_of(c * 512, 512)
    other_half = pl.multiple_of(other * 512, 512)
    for b in range(NB):
        send(qown.at[b, :, pl.ds(other_half, 512)], q0recv.at[b], ssem.at[Q0, b], rsem.at[Q0, b], partner)

    def q1(b):
        got(q0recv.at[b], rsem.at[Q0, b])
        mine = qown[b, :, pl.ds(half, 512)]
        x = jnp.where(head_core == c, mine, q0recv[b])
        for k in range(4):
            cand[b, k] = x[:, k * HD : (k + 1) * HD]
        q1recv[b, z] = cand[b, z]
        for d in (1, 3, 2):
            zz, dev = zpeer(d)
            send(cand.at[b, zz], q1recv.at[b, z], ssem.at[Q1, b], rsem.at[Q1, b], dev)

    def q2(b):
        got(q1recv.at[b, pl.ds(0, 3)], rsem.at[Q1, b])
        x = q1recv[b, 0]
        for k in range(1, 4):
            x = jnp.where(head_chip == k, q1recv[b, k], x)
        qall[b, 4 * c + z] = x
        for d in (1, 3, 2):
            _, dev = zpeer(d)
            piece = qall.at[b, 4 * c + z]
            send(piece, piece, ssem.at[Q2, b], rsem.at[Q2, b], dev)

    def q3(b):
        got(q1recv.at[b, pl.ds(0, 3)], rsem.at[Q2, b])
        piece = qall.at[b, pl.ds(4 * c, 4)]
        send(piece, piece, ssem.at[Q3, b], rsem.at[Q3, b], partner)

    def q4(b):
        got(qall.at[b, pl.ds(4 * other, 4)], rsem.at[Q3, b])

    S, PR, M = (s0, s1), (p0, p1), (ms0, ms1)
    row_of = lax.broadcasted_iota(jnp.int32, (TILE, HD), 0)
    lane_of = lax.broadcasted_iota(jnp.int32, (TILE, HD), 1)
    hot = jnp.where(row_of % QT == lane_of, 1.0, 0.0).astype(BF16)
    diag = row_of[:HD] == lane_of[:HD]

    def to_lanes(x):
        return jnp.sum(jnp.where(diag, x, 0.0), axis=0, keepdims=True)

    def to_rows(x):
        return jnp.sum(jnp.where(diag, jnp.broadcast_to(x, (HD, HD)), 0.0), axis=1, keepdims=True)

    def make_bias(b):
        start = t * length - (len_ref[b] - QT)
        pos = lax.broadcasted_iota(jnp.int32, (length, HD), 0) + start
        col = lax.broadcasted_iota(jnp.int32, (length, HD), 1)
        kx[...] = jnp.where(pos > col, MASKED, 0.0).astype(BF16)

    def qk(b, r):
        q = jnp.concatenate([qall[b, pl.ds(4 * r, 4)].reshape(TILE, HD), hot], axis=1)
        top = None
        for k in range(length // 512):
            keys = jnp.concatenate([kv[b, k * 512 : (k + 1) * 512, :HD], kx[k * 512 : (k + 1) * 512, :]], axis=1)
            x = lax.dot_general(q, keys, (((1,), (1,)), ((), ())), preferred_element_type=F32)
            S[r][:, k * 512 : (k + 1) * 512] = x
            for j in range(4):
                part = x[:, j * HD : (j + 1) * HD]
                top = part if top is None else jnp.maximum(top, part)
        m = jnp.broadcast_to(jnp.max(top, axis=1, keepdims=True), (TILE, HD))
        M[r][...] = m
        for u in range(2):
            mlbuf[b, 2 * r + u : 2 * r + u + 1, :] = to_lanes(m[u * HD : (u + 1) * HD])

    def weigh(r):
        m = M[r][...]
        for k in range(length // HD):
            x = S[r][:, k * HD : (k + 1) * HD]
            PR[r][:, k * HD : (k + 1) * HD] = jnp.exp2((x - m) * EXP2_SCALE).astype(BF16)

    def pv(b, r):
        vals = jnp.concatenate([kv[b, :, HD:], jnp.ones((length, HD), BF16)], axis=1)
        acc = jnp.dot(PR[r][...], vals, preferred_element_type=F32)
        oacc[b, r * TILE : (r + 1) * TILE, :] = acc[:, :HD]
        for u in range(2):
            mlbuf[b, 4 + 2 * r + u : 5 + 2 * r + u, :] = to_lanes(acc[u * HD : (u + 1) * HD, HD:])

    def ml(b):
        mlrecv[b, t] = mlbuf[b]
        for d in range(1, 8):
            send(mlbuf.at[b], mlrecv.at[b, t], ssem.at[ML, b], rsem.at[ML, b], {"tp": (t + d) % 8})

    def c1(b):
        got(mlrecv.at[b, pl.ds(0, 7)], rsem.at[ML, b])
        every = mlrecv[b]
        maxima = every[:, :4, :]
        top = jnp.max(maxima, axis=0)
        total = jnp.sum(every[:, 4:, :] * jnp.exp2((maxima - top[None]) * EXP2_SCALE), axis=0)
        scale = jnp.exp2((mlbuf[b, :4, :] - top) * EXP2_SCALE) / total
        for u in range(4):
            o = oacc[b, u * HD : (u + 1) * HD, :] * to_rows(scale[u : u + 1])
            osend[b, 2 * u : 2 * u + 2] = o.astype(BF16).reshape(2, QT, HD)
        c1recv[b, s] = osend[b, s]
        for d in range(1, 8):
            ss = (s + d) % 8
            send(osend.at[b, ss], c1recv.at[b, s], ssem.at[C1, b], rsem.at[C1, b], {"seq": ss})

    def pick(pieces, index):
        x = pieces[0]
        for k in range(1, len(pieces)):
            x = jnp.where(index == k, pieces[k], x)
        return x

    def c2(b):
        got(c1recv.at[b, pl.ds(0, 7)], rsem.at[C1, b])
        pieces = [c1recv[b, k] for k in range(KVH)]
        for k in range(4):
            c2send[b, k] = pick(pieces, other_slots[k])
        send(c2send.at[b], c2recv.at[b], ssem.at[C2, b], rsem.at[C2, b], partner)

    def c3(b):
        got(c2recv.at[b], rsem.at[C2, b])
        pieces = [c1recv[b, k] for k in range(KVH)]
        for k in range(4):
            x = pick(pieces, my_slots[k]).astype(F32) + c2recv[b, k].astype(F32)
            psum[b, k] = x.astype(BF16)
        c3recv[b, z] = psum[b, z]
        for d in (1, 3, 2):
            zz, dev = zpeer(d)
            send(psum.at[b, zz], c3recv.at[b, z], ssem.at[C3, b], rsem.at[C3, b], dev)

    def c4(b):
        got(c3recv.at[b, pl.ds(0, 3)], rsem.at[C3, b])
        attall[s, b] = jnp.sum(c3recv[b].astype(F32), axis=0).astype(BF16)
        for d in range(1, 8):
            piece = attall.at[s, b]
            send(piece, piece, ssem.at[C4, b], rsem.at[C4, b], {"seq": (s + d) % 8})

    def c5(b):
        got(c1recv.at[b, pl.ds(0, 7)], rsem.at[C4, b])

    for step, b in (
        (q1, 0), (q1, 1), (q1, 2), (q2, 0), (q1, 3), (q2, 1), (q1, 4), (q3, 0), (q2, 2), (q1, 5), (q3, 1), (q2, 3), (q4, 0),
    ):
        step(b)
    kv_load(0).wait()
    make_bias(0)
    qk(0, 0)

    def guarded(step, b):
        pl.when((b >= 0) & (b < NB))(lambda: step(b))

    def body(b, carry):
        for step, lead in ((q4, 1), (q3, 2), (q2, 4), (q1, 6)):
            guarded(step, b + lead)
        qk(b, 1)
        weigh(0)
        pv(jnp.maximum(b - 1, 0), 1)
        for step, lag in ((ml, 1), (c1, 3), (c2, 6), (c3, 7)):
            guarded(step, b - lag)
        after = jnp.minimum(b + 1, NB - 1)
        pl.when(b + 1 < NB)(lambda: kv_load(after).wait())
        make_bias(after)
        qk(after, 0)
        weigh(1)
        pv(b, 0)
        return carry

    lax.fori_loop(0, NB, body, 0)
    pv(NB - 1, 1)
    for step, b in (
        (ml, 7), (c1, 5), (c2, 2), (c3, 1), (c4, 0), (c1, 6), (c2, 3), (c3, 2), (c4, 1), (c1, 7), (c2, 4), (c3, 3), (c4, 2),
        (c2, 5), (c3, 4), (c4, 3), (c2, 6), (c3, 5), (c4, 4), (c2, 7), (c3, 6), (c4, 5), (c3, 7), (c4, 6), (c4, 7),
    ):
        step(b)
    for b in range(NB):
        c5(b)
    wload.wait()

    wide = w.shape[1] // NCH

    def project(n):
        x = jnp.concatenate([attall[j].reshape(ROWS, HD) for j in range(GS)], axis=1)
        y = jnp.dot(x, w[:, n * wide : (n + 1) * wide], preferred_element_type=F32).astype(BF16)
        for b in range(NB):
            ybuf[n, b % 2, b // 2] = y[b * QT : (b + 1) * QT]
        send(ybuf.at[n, other], d1recv.at[n], dssem.at[0, n], drsem.at[0, n], partner)

    def reduce_pair(n):
        got(d1recv.at[n], drsem.at[0, n])
        x = ybuf[n, c].astype(F32) + d1recv[n].astype(F32)
        d2send[n] = x.astype(BF16)
        d2recv[n, z] = d2send[n, z]
        for d in (1, 3, 2):
            zz, dev = zpeer(d)
            send(d2send.at[n, zz], d2recv.at[n, z], dssem.at[1, n], drsem.at[1, n], dev)

    def finish(n):
        got(d2recv.at[n, pl.ds(0, 3)], drsem.at[1, n])
        out_ref[0, :, n * wide : (n + 1) * wide] = jnp.sum(d2recv[n].astype(F32), axis=0).astype(BF16)

    project(0)
    project(1)
    reduce_pair(0)
    project(2)
    reduce_pair(1)
    project(3)
    reduce_pair(2)
    reduce_pair(3)

    def drain(b, carry):
        sent(q0recv.at[b], ssem.at[Q0, b])
        sent(q1recv.at[b, pl.ds(0, 3)], ssem.at[Q1, b])
        sent(q1recv.at[b, pl.ds(0, 3)], ssem.at[Q2, b])
        sent(qall.at[b, pl.ds(0, 4)], ssem.at[Q3, b])
        sent(mlrecv.at[b, pl.ds(0, 7)], ssem.at[ML, b])
        sent(c1recv.at[b, pl.ds(0, 7)], ssem.at[C1, b])
        sent(c2send.at[b], ssem.at[C2, b])
        sent(c3recv.at[b, pl.ds(0, 3)], ssem.at[C3, b])
        sent(c1recv.at[b, pl.ds(0, 7)], ssem.at[C4, b])
        return carry

    lax.fori_loop(0, NB, drain, 0)
    for n in range(NCH):
        sent(d1recv.at[n], dssem.at[0, n])
        sent(d2recv.at[n, pl.ds(0, 3)], dssem.at[1, n])
    for n in range(NCH):
        finish(n)


def local(query, cache, head_of_slot, lengths, out_weight):
    length = cache.shape[1]
    entries = cache.reshape(NB, length, 2 * HD)
    wide = out_weight.shape[1]
    vm = pltpu.VMEM
    dma = pltpu.SemaphoreType.DMA
    smem = pl.BlockSpec(memory_space=pltpu.SMEM)
    anywhere = pl.BlockSpec(memory_space=pl.ANY)
    return pl.pallas_call(
        kernel,
        out_shape=jax.ShapeDtypeStruct((1, QT, wide), BF16),
        in_specs=[smem, smem, anywhere, anywhere, anywhere],
        out_specs=pl.BlockSpec(memory_space=pltpu.VMEM),
        scratch_shapes=[
            vm((NB, QT, GS * HD), BF16),
            vm((NB, QT, 4 * HD), BF16),
            vm((NB, 4, QT, HD), BF16),
            vm((NB, 4, QT, HD), BF16),
            vm((NB, GS, QT, HD), BF16),
            vm((NB, length, 2 * HD), BF16),
            vm(out_weight.shape, BF16),
            vm((length, HD), BF16),
            vm((TILE, length), F32),
            vm((TILE, length), F32),
            vm((TILE, length), BF16),
            vm((TILE, length), BF16),
            vm((TILE, HD), F32),
            vm((TILE, HD), F32),
            vm((NB, ROWS, HD), F32),
            vm((NB, 8, HD), F32),
            vm((NB, 8, 8, HD), F32),
            vm((NB, GS, QT, HD), BF16),
            vm((NB, GS, QT, HD), BF16),
            vm((NB, 4, QT, HD), BF16),
            vm((NB, 4, QT, HD), BF16),
            vm((NB, 4, QT, HD), BF16),
            vm((NB, 4, QT, HD), BF16),
            vm((GS, NB, QT, HD), BF16),
            vm((NCH, 2, 4, QT, wide // NCH), BF16),
            vm((NCH, 4, QT, wide // NCH), BF16),
            vm((NCH, 4, QT, wide // NCH), BF16),
            vm((NCH, 4, QT, wide // NCH), BF16),
            dma((9, NB)),
            dma((9, NB)),
            dma((2, NCH)),
            dma((2, NCH)),
            dma((NB + 2,)),
        ],
        compiler_params=pltpu.CompilerParams(
            collective_id=0, has_side_effects=True, vmem_limit_bytes=58 * 2**20
        ),
        name="attend",
    )(head_of_slot, lengths, query, entries, out_weight)


def solution(mesh):
    in_specs = (
        P("grp", None, "tp"),
        P("grp", "tp", "seq", None),
        P("grp"),
        P("grp"),
        P("tp", "seq"),
    )
    out_specs = P(("grp", "tp"), None, "seq")
    return jax.shard_map(local, mesh=mesh, in_specs=in_specs, out_specs=out_specs, check_vma=False)
```

```python
import functools
import math

import jax
import jax.numpy as jnp
from jax import lax
from jax.experimental import pallas as pl
from jax.experimental.pallas import tpu as pltpu
from jax.sharding import PartitionSpec as P

HQ = 64
KVH = 8
HD = 128
NB = 8
QT = 64
GS = 8
ROWS = GS * QT
TILE = 256
MASKED = -1e30
EXP2_SCALE = math.log2(math.e) / math.sqrt(HD)
F32 = jnp.float32
BF16 = jnp.bfloat16
MESH = pl.DeviceIdType.MESH
Q0, Q1, Q2, Q3, C1, C1M, C3, C3M, C4 = range(9)


def kernel(
    heads_ref, len_ref, q_hbm, kv_hbm, w_hbm, out_ref,
    qown, q0recv, cand, q1recv, qall, kv, w, s0, s1, p0, p1, m0, m1,
    osend, mlbuf, c1recv, c1ml, c3send, c3sml, c3recv, c3ml, attall,
    ysend, yown, d1recv, d2send, d2recv, ssem, rsem, dssem, drsem, lsem,
):
    s = lax.axis_index("seq")
    t = lax.axis_index("tp")
    z = t // 2
    c = t % 2
    other = 1 - c
    length = kv.shape[1]
    head = heads_ref[s]
    head_chip = head // 2
    head_core = head % 2

    def slot_of(h):
        slot = jnp.int32(0)
        for k in range(KVH):
            slot = jnp.where(heads_ref[k] == h, k, slot)
        return slot

    slots = [slot_of(k) for k in range(KVH)]
    partner = {"tp": t + 1 - 2 * c}

    def zpeer(d):
        zz = (z + d) % 4
        return zz, {"tp": 2 * zz + c}

    def send(src, dst, ss, rs, dev):
        pltpu.make_async_remote_copy(
            src_ref=src, dst_ref=dst, send_sem=ss, recv_sem=rs, device_id=dev, device_id_type=MESH
        ).start()

    def got(ref, rs):
        pltpu.make_async_remote_copy(
            src_ref=ref, dst_ref=ref, send_sem=rs, recv_sem=rs, device_id=partner, device_id_type=MESH
        ).wait_recv()

    def sent(ref, ss):
        pltpu.make_async_remote_copy(
            src_ref=ref, dst_ref=ref, send_sem=ss, recv_sem=ss, device_id=partner, device_id_type=MESH
        ).wait_send()

    barrier = pltpu.get_barrier_semaphore()
    for d in range(1, 8):
        pl.semaphore_signal(barrier, inc=1, device_id={"tp": (t + d) % 8}, device_id_type=MESH)
        pl.semaphore_signal(barrier, inc=1, device_id={"seq": (s + d) % 8}, device_id_type=MESH)

    qload = pltpu.make_async_copy(q_hbm, qown, lsem.at[NB])
    qload.start()

    def kv_load(b):
        return pltpu.make_async_copy(kv_hbm.at[b], kv.at[b], lsem.at[b])

    wload = pltpu.make_async_copy(w_hbm, w, lsem.at[NB + 1])
    qload.wait()
    for b in range(NB):
        kv_load(b).start()
    wload.start()
    pl.semaphore_wait(barrier, 14)

    half = pl.multiple_of(c * 512, 512)
    other_half = pl.multiple_of(other * 512, 512)
    for b in range(NB):
        send(qown.at[b, :, pl.ds(other_half, 512)], q0recv.at[b], ssem.at[Q0, b], rsem.at[Q0, b], partner)

    def q1(b):
        got(q0recv.at[b], rsem.at[Q0, b])
        mine = qown[b, :, pl.ds(half, 512)]
        x = jnp.where(head_core == c, mine, q0recv[b])
        for k in range(4):
            cand[b, k] = x[:, k * HD : (k + 1) * HD]
        q1recv[b, z] = cand[b, z]
        for d in (2, 1, 3):
            zz, dev = zpeer(d)
            send(cand.at[b, zz], q1recv.at[b, z], ssem.at[Q1, b], rsem.at[Q1, b], dev)

    def q2(b):
        got(q1recv.at[b, pl.ds(0, 3)], rsem.at[Q1, b])
        qall[b, 4 * c + z] = pick([q1recv[b, k] for k in range(4)], head_chip)
        for d in (2, 1, 3):
            _, dev = zpeer(d)
            piece = qall.at[b, 4 * c + z]
            send(piece, piece, ssem.at[Q2, b], rsem.at[Q2, b], dev)

    def q3(b):
        got(q1recv.at[b, pl.ds(0, 3)], rsem.at[Q2, b])
        piece = qall.at[b, pl.ds(4 * c, 4)]
        send(piece, piece, ssem.at[Q3, b], rsem.at[Q3, b], partner)

    def q4(b):
        got(qall.at[b, pl.ds(4 * other, 4)], rsem.at[Q3, b])

    def pick(pieces, index):
        x = pieces[0]
        for k in range(1, len(pieces)):
            x = jnp.where(index == k, pieces[k], x)
        return x

    S, PR, M = (s0, s1), (p0, p1), (m0, m1)
    first = (4 * c, 4 * other)
    row_of = lax.broadcasted_iota(jnp.int32, (TILE, HD), 0)
    lane_of = lax.broadcasted_iota(jnp.int32, (TILE, HD), 1)
    hot = jnp.where(row_of % QT == lane_of, 1.0, 0.0).astype(BF16)
    ahead = (row_of[:HD] - lane_of[:HD]).astype(F32).astype(BF16)
    row, lane = row_of[:QT], lane_of[:QT]

    def bias(start, k):
        edge = jnp.clip(start - HD * k, -200, 200).astype(F32)
        edge = jnp.full((HD, HD), edge, F32).astype(BF16)
        return jnp.where(ahead > edge, jnp.asarray(MASKED, BF16), jnp.asarray(0, BF16))

    def qk(b, r):
        start = len_ref[b] - QT - t * length
        q = jnp.concatenate([qall[b, pl.ds(first[r], 4)].reshape(TILE, HD), hot], axis=1)
        top = None
        for k in range(length // 512):
            extra = jnp.concatenate([bias(start, 4 * k + i) for i in range(4)], axis=0)
            keys = jnp.concatenate([kv[b, k * 512 : (k + 1) * 512, :HD], extra], axis=1)
            x = lax.dot_general(q, keys, (((1,), (1,)), ((), ())), preferred_element_type=F32)
            S[r][:, k * 512 : (k + 1) * 512] = x
            for j in range(4):
                part = x[:, j * HD : (j + 1) * HD]
                top = part if top is None else jnp.maximum(top, part)
        M[r][...] = jnp.broadcast_to(jnp.max(top, axis=1, keepdims=True), (TILE, HD))

    def weigh(r):
        m = M[r][...]
        for k in range(length // HD):
            x = S[r][:, k * HD : (k + 1) * HD]
            PR[r][:, k * HD : (k + 1) * HD] = jnp.exp2((x - m) * EXP2_SCALE).astype(BF16)

    def pv(b, r):
        vals = jnp.concatenate([kv[b, :, HD:], jnp.ones((length, HD), BF16)], axis=1)
        acc = jnp.dot(PR[r][...], vals, preferred_element_type=F32)
        m = M[r][...]
        osend[b, pl.ds(first[r], 4)] = acc[:, :HD].astype(BF16).reshape(4, QT, HD)
        for j in range(4):
            rows = slice(j * QT, (j + 1) * QT)
            x = jnp.where(lane == row, m[rows], 0.0) + jnp.where(lane == row + QT, acc[rows, HD:], 0.0)
            mlbuf[b, first[r] + j] = jnp.sum(x, axis=0, keepdims=True)

    def to_rows(x):
        return jnp.sum(jnp.where(lane == row, jnp.broadcast_to(x, (QT, HD)), 0.0), axis=1, keepdims=True)

    def c1(b):
        c1recv[b, s] = osend[b, s]
        c1ml[b, s] = mlbuf[b, s]
        for d in (6, 2, 3, 5, 7, 1, 4):
            ss = (s + d) % 8
            send(osend.at[b, ss], c1recv.at[b, s], ssem.at[C1, b], rsem.at[C1, b], {"seq": ss})
            send(mlbuf.at[b, ss], c1ml.at[b, s], ssem.at[C1M, b], rsem.at[C1M, b], {"seq": ss})

    def c3(b):
        got(c1recv.at[b, pl.ds(0, 7)], rsem.at[C1, b])
        got(c1ml.at[b, pl.ds(0, 7)], rsem.at[C1M, b])
        pieces = [c1recv[b, k] for k in range(KVH)]
        rows = [c1ml[b, k] for k in range(KVH)]
        for k in range(KVH):
            c3send[b, k] = pick(pieces, slots[k])
            c3sml[b, k] = pick(rows, slots[k])
        c3recv[b, t] = c3send[b, t]
        c3ml[b, t] = c3sml[b, t]
        for d in (4, 5, 3, 2, 6, 7, 1):
            tt = (t + d) % 8
            send(c3send.at[b, tt], c3recv.at[b, t], ssem.at[C3, b], rsem.at[C3, b], {"tp": tt})
            send(c3sml.at[b, tt], c3ml.at[b, t], ssem.at[C3M, b], rsem.at[C3M, b], {"tp": tt})

    def c4(b):
        got(c3recv.at[b, pl.ds(0, 7)], rsem.at[C3, b])
        got(c3ml.at[b, pl.ds(0, 7)], rsem.at[C3M, b])
        ml = c3ml[b].reshape(8, HD)
        top = jnp.max(ml, axis=0, keepdims=True)
        scale = jnp.exp2((ml - top) * EXP2_SCALE)
        total = jnp.sum(ml * pltpu.roll(scale, QT, 1), axis=0, keepdims=True)
        scale = scale / pltpu.roll(jnp.broadcast_to(total, (8, HD)), QT, 1)
        x = c3recv[b, 0].astype(F32) * to_rows(scale[:1])
        for k in range(1, 8):
            x = x + c3recv[b, k].astype(F32) * to_rows(scale[k : k + 1])
        attall[b, s] = x.astype(BF16)
        for d in (6, 2, 3, 5, 7, 1, 4):
            piece = attall.at[b, s]
            send(piece, piece, ssem.at[C4, b], rsem.at[C4, b], {"seq": (s + d) % 8})

    def c5(b):
        got(c1recv.at[b, pl.ds(0, 7)], rsem.at[C4, b])
        x = jnp.concatenate([attall[b, j] for j in range(GS)], axis=1)
        y = jnp.dot(x, w[...], preferred_element_type=F32)

        @pl.when(c == b % 2)
        def _():
            yown[...] = y

        @pl.when(c != b % 2)
        def _():
            ysend[b // 2] = y.astype(BF16)
            send(ysend.at[b // 2], d1recv.at[b // 2], dssem.at[0, b // 2], drsem.at[0, b // 2], partner)

    def d2(b):
        k = b // 2

        @pl.when(c == b % 2)
        def _():
            got(d1recv.at[k], drsem.at[0, k])
            d2send[k] = (yown[...] + d1recv[k].astype(F32)).astype(BF16)

            @pl.when(z == k)
            def _():
                d2recv[k] = d2send[k]

            @pl.when(z != k)
            def _():
                send(d2send.at[k], d2recv.at[z], dssem.at[1, k], drsem.at[1, 0], {"tp": b})

    for step, b in (
        (q1, 0), (q1, 1), (q1, 2), (q2, 0), (q1, 3), (q2, 1), (q1, 4), (q3, 0), (q2, 2),
    ):
        step(b)
    kv_load(0).wait()
    qk(0, 0)

    def guarded(step, b):
        pl.when((b >= 0) & (b < NB))(lambda: step(b))

    def body(b, carry):
        for step, lead in ((q4, 0), (q3, 1), (q2, 3), (q1, 5), (c1, -1), (c3, -4), (c4, -7)):
            guarded(step, b + lead)
        after = jnp.minimum(b + 1, NB - 1)
        pl.when(b + 1 < NB)(lambda: kv_load(after).wait())
        qk(b, 1)
        weigh(0)
        pv(b, 0)
        weigh(1)
        qk(after, 0)
        pv(b, 1)
        return carry

    lax.fori_loop(0, NB, body, 0)
    c1(7)
    wload.wait()
    for step, b in (
        (c3, 4), (c4, 1), (c3, 5), (c4, 2), (c5, 0), (c3, 6), (c4, 3), (d2, 0), (c5, 1), (c3, 7), (c4, 4), (d2, 1), (c5, 2),
        (c4, 5), (d2, 2), (c5, 3), (c4, 6), (d2, 3), (c5, 4), (d2, 4), (c4, 7), (c5, 5), (d2, 5), (c5, 6), (d2, 6), (c5, 7), (d2, 7),
    ):
        step(b)
    got(d2recv.at[pl.ds(0, 3)], drsem.at[1, 0])
    out_ref[0] = jnp.sum(d2recv[...].astype(F32), axis=0).astype(BF16)

    def drain(b, carry):
        sent(q0recv.at[b], ssem.at[Q0, b])
        sent(q1recv.at[b, pl.ds(0, 3)], ssem.at[Q1, b])
        sent(q1recv.at[b, pl.ds(0, 3)], ssem.at[Q2, b])
        sent(qall.at[b, pl.ds(0, 4)], ssem.at[Q3, b])
        for k in (C1, C3, C4):
            sent(c1recv.at[b, pl.ds(0, 7)], ssem.at[k, b])
        for k in (C1M, C3M):
            sent(c1ml.at[b, pl.ds(0, 7)], ssem.at[k, b])
        return carry

    lax.fori_loop(0, NB, drain, 0)
    for k in range(4):
        sent(d1recv.at[k], dssem.at[0, k])
        pl.when(z != k)(lambda k=k: sent(d2send.at[k], dssem.at[1, k]))


def local(query, cache, head_of_slot, lengths, out_weight):
    length = cache.shape[1]
    entries = cache.reshape(NB, length, 2 * HD)
    wide = out_weight.shape[1]
    vm = pltpu.VMEM
    dma = pltpu.SemaphoreType.DMA
    smem = pl.BlockSpec(memory_space=pltpu.SMEM)
    anywhere = pl.BlockSpec(memory_space=pl.ANY)
    return pl.pallas_call(
        kernel,
        out_shape=jax.ShapeDtypeStruct((1, QT, wide), BF16),
        in_specs=[smem, smem, anywhere, anywhere, anywhere],
        out_specs=pl.BlockSpec(memory_space=pltpu.VMEM),
        scratch_shapes=[
            vm((NB, QT, GS * HD), BF16),
            vm((NB, QT, 4 * HD), BF16),
            vm((NB, 4, QT, HD), BF16),
            vm((NB, 4, QT, HD), BF16),
            vm((NB, GS, QT, HD), BF16),
            vm((NB, length, 2 * HD), BF16),
            vm(out_weight.shape, BF16),
            vm((TILE, length), F32),
            vm((TILE, length), F32),
            vm((TILE, length), BF16),
            vm((TILE, length), BF16),
            vm((TILE, HD), F32),
            vm((TILE, HD), F32),
            vm((NB, GS, QT, HD), BF16),
            vm((NB, GS, 1, HD), F32),
            vm((NB, KVH, QT, HD), BF16),
            vm((NB, KVH, 1, HD), F32),
            vm((NB, KVH, QT, HD), BF16),
            vm((NB, KVH, 1, HD), F32),
            vm((NB, 8, QT, HD), BF16),
            vm((NB, 8, 1, HD), F32),
            vm((NB, GS, QT, HD), BF16),
            vm((4, QT, wide), BF16),
            vm((QT, wide), F32),
            vm((4, QT, wide), BF16),
            vm((4, QT, wide), BF16),
            vm((4, QT, wide), BF16),
            dma((9, NB)),
            dma((9, NB)),
            dma((2, 4)),
            dma((2, 4)),
            dma((NB + 2,)),
        ],
        compiler_params=pltpu.CompilerParams(
            collective_id=0, has_side_effects=True, vmem_limit_bytes=58 * 2**20
        ),
        name="attend",
    )(head_of_slot, lengths, query, entries, out_weight)


def solution(mesh):
    in_specs = (
        P("grp", None, "tp"),
        P("grp", "tp", "seq", None),
        P("grp"),
        P("grp"),
        P("tp", "seq"),
    )
    out_specs = P(("grp", "tp"), None, "seq")
    return jax.shard_map(local, mesh=mesh, in_specs=in_specs, out_specs=out_specs, check_vma=False)
```

```python
import functools
import math

import jax
import jax.numpy as jnp
from jax import lax
from jax.experimental import pallas as pl
from jax.experimental.pallas import tpu as pltpu
from jax.sharding import PartitionSpec as P

HQ = 64
KVH = 8
HD = 128
NB = 8
QT = 64
GS = 8
ROWS = GS * QT
TILE = 256
MASKED = -1e30
EXP2_SCALE = math.log2(math.e) / math.sqrt(HD)
F32 = jnp.float32
BF16 = jnp.bfloat16
MESH = pl.DeviceIdType.MESH
Q0, Q1, Q2, Q3, C1, C1M, C3, C3M, C4 = range(9)


def kernel(
    heads_ref, len_ref, q_hbm, kv_hbm, w_hbm, out_ref,
    qown, q0recv, cand, q1recv, qall, kv, w, s0, s1, p0, p1, m0, m1,
    osend, mlbuf, c1recv, c1ml, c3send, c3sml, c3recv, c3ml, attall,
    ysend, yown, d1recv, d2send, d2recv, ssem, rsem, dssem, drsem, lsem,
):
    s = lax.axis_index("seq")
    t = lax.axis_index("tp")
    z = t // 2
    c = t % 2
    other = 1 - c
    length = kv.shape[1]
    head = heads_ref[s]
    head_chip = head // 2
    head_core = head % 2

    def slot_of(h):
        slot = jnp.int32(0)
        for k in range(KVH):
            slot = jnp.where(heads_ref[k] == h, k, slot)
        return slot

    slots = [slot_of(k) for k in range(KVH)]
    partner = {"tp": t + 1 - 2 * c}

    def zpeer(d):
        zz = (z + d) % 4
        return zz, {"tp": 2 * zz + c}

    def send(src, dst, ss, rs, dev):
        pltpu.make_async_remote_copy(
            src_ref=src, dst_ref=dst, send_sem=ss, recv_sem=rs, device_id=dev, device_id_type=MESH
        ).start()

    def got(ref, rs):
        pltpu.make_async_remote_copy(
            src_ref=ref, dst_ref=ref, send_sem=rs, recv_sem=rs, device_id=partner, device_id_type=MESH
        ).wait_recv()

    def sent(ref, ss):
        pltpu.make_async_remote_copy(
            src_ref=ref, dst_ref=ref, send_sem=ss, recv_sem=ss, device_id=partner, device_id_type=MESH
        ).wait_send()

    barrier = pltpu.get_barrier_semaphore()
    for d in range(1, 8):
        pl.semaphore_signal(barrier, inc=1, device_id={"tp": (t + d) % 8}, device_id_type=MESH)
        pl.semaphore_signal(barrier, inc=1, device_id={"seq": (s + d) % 8}, device_id_type=MESH)

    qload = pltpu.make_async_copy(q_hbm, qown, lsem.at[NB])
    qload.start()

    def kv_load(b):
        return pltpu.make_async_copy(kv_hbm.at[b], kv.at[b], lsem.at[b])

    wload = pltpu.make_async_copy(w_hbm, w, lsem.at[NB + 1])
    qload.wait()
    for b in range(NB):
        kv_load(b).start()
    wload.start()
    pl.semaphore_wait(barrier, 14)

    half = pl.multiple_of(c * 512, 512)
    other_half = pl.multiple_of(other * 512, 512)
    for b in range(NB):
        send(qown.at[b, :, pl.ds(other_half, 512)], q0recv.at[b], ssem.at[Q0, b], rsem.at[Q0, b], partner)

    def q1(b):
        got(q0recv.at[b], rsem.at[Q0, b])
        mine = qown[b, :, pl.ds(half, 512)]
        x = jnp.where(head_core == c, mine, q0recv[b])
        for k in range(4):
            cand[b, k] = x[:, k * HD : (k + 1) * HD]
        q1recv[b, z] = cand[b, z]
        for d in (2, 1, 3):
            zz, dev = zpeer(d)
            send(cand.at[b, zz], q1recv.at[b, z], ssem.at[Q1, b], rsem.at[Q1, b], dev)

    def q2(b):
        got(q1recv.at[b, pl.ds(0, 3)], rsem.at[Q1, b])
        qall[b, 4 * c + z] = pick([q1recv[b, k] for k in range(4)], head_chip)
        for d in (2, 1, 3):
            _, dev = zpeer(d)
            piece = qall.at[b, 4 * c + z]
            send(piece, piece, ssem.at[Q2, b], rsem.at[Q2, b], dev)

    def q3(b):
        got(q1recv.at[b, pl.ds(0, 3)], rsem.at[Q2, b])
        piece = qall.at[b, pl.ds(4 * c, 4)]
        send(piece, piece, ssem.at[Q3, b], rsem.at[Q3, b], partner)

    def q4(b):
        got(qall.at[b, pl.ds(4 * other, 4)], rsem.at[Q3, b])

    def pick(pieces, index):
        x = pieces[0]
        for k in range(1, len(pieces)):
            x = jnp.where(index == k, pieces[k], x)
        return x

    S, PR, M = (s0, s1), (p0, p1), (m0, m1)
    first = (4 * c, 4 * other)
    row_of = lax.broadcasted_iota(jnp.int32, (TILE, HD), 0)
    lane_of = lax.broadcasted_iota(jnp.int32, (TILE, HD), 1)
    hot = jnp.where(row_of % QT == lane_of, 1.0, 0.0).astype(BF16)
    ahead = (row_of[:HD] - lane_of[:HD]).astype(F32).astype(BF16)
    row, lane = row_of[:QT], lane_of[:QT]

    def bias(start, k):
        edge = jnp.clip(start - HD * k, -200, 200).astype(F32)
        edge = jnp.full((HD, HD), edge, F32).astype(BF16)
        return jnp.where(ahead > edge, jnp.asarray(MASKED, BF16), jnp.asarray(0, BF16))

    def qk(b, r):
        start = len_ref[b] - QT - t * length
        q = jnp.concatenate([qall[b, pl.ds(first[r], 4)].reshape(TILE, HD), hot], axis=1)
        top = None
        for k in range(length // 512):
            extra = jnp.concatenate([bias(start, 4 * k + i) for i in range(4)], axis=0)
            keys = jnp.concatenate([kv[b, k * 512 : (k + 1) * 512, :HD], extra], axis=1)
            x = lax.dot_general(q, keys, (((1,), (1,)), ((), ())), preferred_element_type=F32)
            S[r][:, k * 512 : (k + 1) * 512] = x
            for j in range(4):
                part = x[:, j * HD : (j + 1) * HD]
                top = part if top is None else jnp.maximum(top, part)
        M[r][...] = jnp.broadcast_to(jnp.max(top, axis=1, keepdims=True), (TILE, HD))

    def weigh(r):
        m = M[r][...]
        for k in range(length // HD):
            x = S[r][:, k * HD : (k + 1) * HD]
            PR[r][:, k * HD : (k + 1) * HD] = jnp.exp2((x - m) * EXP2_SCALE).astype(BF16)

    def pv(b, r):
        vals = jnp.concatenate([kv[b, :, HD:], jnp.ones((length, HD), BF16)], axis=1)
        acc = jnp.dot(PR[r][...], vals, preferred_element_type=F32)
        m = M[r][...]
        osend[b, pl.ds(first[r], 4)] = acc[:, :HD].astype(BF16).reshape(4, QT, HD)
        for j in range(4):
            rows = slice(j * QT, (j + 1) * QT)
            x = jnp.where(lane == row, m[rows], 0.0) + jnp.where(lane == row + QT, acc[rows, HD:], 0.0)
            mlbuf[b, first[r] + j] = jnp.sum(x, axis=0, keepdims=True)

    def to_rows(x):
        return jnp.sum(jnp.where(lane == row, jnp.broadcast_to(x, (QT, HD)), 0.0), axis=1, keepdims=True)

    def c1(b):
        c1recv[b, s] = osend[b, s]
        c1ml[b, s] = mlbuf[b, s]
        for d in (6, 2, 3, 5, 7, 1, 4):
            ss = (s + d) % 8
            send(osend.at[b, ss], c1recv.at[b, s], ssem.at[C1, b], rsem.at[C1, b], {"seq": ss})
            send(mlbuf.at[b, ss], c1ml.at[b, s], ssem.at[C1M, b], rsem.at[C1M, b], {"seq": ss})

    def c3(b):
        got(c1recv.at[b, pl.ds(0, 7)], rsem.at[C1, b])
        got(c1ml.at[b, pl.ds(0, 7)], rsem.at[C1M, b])
        pieces = [c1recv[b, k] for k in range(KVH)]
        rows = [c1ml[b, k] for k in range(KVH)]
        for k in range(KVH):
            c3send[b, k] = pick(pieces, slots[k])
            c3sml[b, k] = pick(rows, slots[k])
        c3recv[b, t] = c3send[b, t]
        c3ml[b, t] = c3sml[b, t]
        for d in (4, 5, 3, 2, 6, 7, 1):
            tt = (t + d) % 8
            send(c3send.at[b, tt], c3recv.at[b, t], ssem.at[C3, b], rsem.at[C3, b], {"tp": tt})
            send(c3sml.at[b, tt], c3ml.at[b, t], ssem.at[C3M, b], rsem.at[C3M, b], {"tp": tt})

    def c4(b):
        got(c3recv.at[b, pl.ds(0, 7)], rsem.at[C3, b])
        got(c3ml.at[b, pl.ds(0, 7)], rsem.at[C3M, b])
        ml = c3ml[b].reshape(8, HD)
        top = jnp.max(ml, axis=0, keepdims=True)
        scale = jnp.exp2((ml - top) * EXP2_SCALE)
        total = jnp.sum(ml * pltpu.roll(scale, QT, 1), axis=0, keepdims=True)
        scale = scale / pltpu.roll(jnp.broadcast_to(total, (8, HD)), QT, 1)
        x = c3recv[b, 0].astype(F32) * to_rows(scale[:1])
        for k in range(1, 8):
            x = x + c3recv[b, k].astype(F32) * to_rows(scale[k : k + 1])
        attall[b, s] = x.astype(BF16)
        for d in (6, 2, 3, 5, 7, 1, 4):
            piece = attall.at[b, s]
            send(piece, piece, ssem.at[C4, b], rsem.at[C4, b], {"seq": (s + d) % 8})

    def c5(b):
        got(c1recv.at[b, pl.ds(0, 7)], rsem.at[C4, b])
        x = jnp.concatenate([attall[b, j] for j in range(GS)], axis=1)
        y = jnp.dot(x, w[...], preferred_element_type=F32)

        @pl.when(c == b % 2)
        def _():
            yown[...] = y

        @pl.when(c != b % 2)
        def _():
            ysend[b // 2] = y.astype(BF16)
            send(ysend.at[b // 2], d1recv.at[b // 2], dssem.at[0, b // 2], drsem.at[0, b // 2], partner)

    def d2(b):
        k = b // 2

        @pl.when(c == b % 2)
        def _():
            got(d1recv.at[k], drsem.at[0, k])
            d2send[k] = (yown[...] + d1recv[k].astype(F32)).astype(BF16)

            @pl.when(z == k)
            def _():
                d2recv[k] = d2send[k]

            @pl.when(z != k)
            def _():
                send(d2send.at[k], d2recv.at[z], dssem.at[1, k], drsem.at[1, 0], {"tp": b})

    for step, b in (
        (q1, 0), (q1, 1), (q2, 0), (q2, 1), (q1, 2), (q3, 0), (q1, 3), (q2, 2), (q1, 4),
    ):
        step(b)
    kv_load(0).wait()
    qk(0, 0)

    def guarded(step, b):
        pl.when((b >= 0) & (b < NB))(lambda: step(b))

    def body(b, carry):
        for step, lead in ((q4, 0), (q3, 1), (q2, 3), (q1, 5), (c1, -1), (c3, -4), (c4, -7)):
            guarded(step, b + lead)
        after = jnp.minimum(b + 1, NB - 1)
        pl.when(b + 1 < NB)(lambda: kv_load(after).wait())
        qk(b, 1)
        weigh(0)
        pv(b, 0)
        weigh(1)
        qk(after, 0)
        pv(b, 1)
        return carry

    lax.fori_loop(0, NB, body, 0)
    c1(7)
    wload.wait()
    for step, b in (
        (c3, 4), (c4, 1), (c4, 2), (c3, 5), (c4, 3), (c3, 6), (c5, 0), (c4, 4), (c3, 7), (d2, 0), (c5, 1), (c4, 5), (d2, 1), (c5, 2),
        (d2, 2), (c4, 6), (c5, 3), (d2, 3), (c4, 7), (c5, 4), (d2, 4), (c5, 5), (d2, 5), (c5, 6), (d2, 6), (c5, 7), (d2, 7),
    ):
        step(b)
    got(d2recv.at[pl.ds(0, 3)], drsem.at[1, 0])
    out_ref[0] = jnp.sum(d2recv[...].astype(F32), axis=0).astype(BF16)

    def drain(b, carry):
        sent(q0recv.at[b], ssem.at[Q0, b])
        sent(q1recv.at[b, pl.ds(0, 3)], ssem.at[Q1, b])
        sent(q1recv.at[b, pl.ds(0, 3)], ssem.at[Q2, b])
        sent(qall.at[b, pl.ds(0, 4)], ssem.at[Q3, b])
        for k in (C1, C3, C4):
            sent(c1recv.at[b, pl.ds(0, 7)], ssem.at[k, b])
        for k in (C1M, C3M):
            sent(c1ml.at[b, pl.ds(0, 7)], ssem.at[k, b])
        return carry

    lax.fori_loop(0, NB, drain, 0)
    for k in range(4):
        sent(d1recv.at[k], dssem.at[0, k])
        pl.when(z != k)(lambda k=k: sent(d2send.at[k], dssem.at[1, k]))


def local(query, cache, head_of_slot, lengths, out_weight):
    length = cache.shape[1]
    entries = cache.reshape(NB, length, 2 * HD)
    wide = out_weight.shape[1]
    vm = pltpu.VMEM
    dma = pltpu.SemaphoreType.DMA
    smem = pl.BlockSpec(memory_space=pltpu.SMEM)
    anywhere = pl.BlockSpec(memory_space=pl.ANY)
    return pl.pallas_call(
        kernel,
        out_shape=jax.ShapeDtypeStruct((1, QT, wide), BF16),
        in_specs=[smem, smem, anywhere, anywhere, anywhere],
        out_specs=pl.BlockSpec(memory_space=pltpu.VMEM),
        scratch_shapes=[
            vm((NB, QT, GS * HD), BF16),
            vm((NB, QT, 4 * HD), BF16),
            vm((NB, 4, QT, HD), BF16),
            vm((NB, 4, QT, HD), BF16),
            vm((NB, GS, QT, HD), BF16),
            vm((NB, length, 2 * HD), BF16),
            vm(out_weight.shape, BF16),
            vm((TILE, length), F32),
            vm((TILE, length), F32),
            vm((TILE, length), BF16),
            vm((TILE, length), BF16),
            vm((TILE, HD), F32),
            vm((TILE, HD), F32),
            vm((NB, GS, QT, HD), BF16),
            vm((NB, GS, 1, HD), F32),
            vm((NB, KVH, QT, HD), BF16),
            vm((NB, KVH, 1, HD), F32),
            vm((NB, KVH, QT, HD), BF16),
            vm((NB, KVH, 1, HD), F32),
            vm((NB, 8, QT, HD), BF16),
            vm((NB, 8, 1, HD), F32),
            vm((NB, GS, QT, HD), BF16),
            vm((4, QT, wide), BF16),
            vm((QT, wide), F32),
            vm((4, QT, wide), BF16),
            vm((4, QT, wide), BF16),
            vm((4, QT, wide), BF16),
            dma((9, NB)),
            dma((9, NB)),
            dma((2, 4)),
            dma((2, 4)),
            dma((NB + 2,)),
        ],
        compiler_params=pltpu.CompilerParams(
            collective_id=0, has_side_effects=True, vmem_limit_bytes=40 * 2**20
        ),
        name="attend",
    )(*[pltpu.with_memory_space_constraint(x, pltpu.HBM) for x in (head_of_slot, lengths, query, entries, out_weight)])


def solution(mesh):
    in_specs = (
        P("grp", None, "tp"),
        P("grp", "tp", "seq", None),
        P("grp"),
        P("grp"),
        P("tp", "seq"),
    )
    out_specs = P(("grp", "tp"), None, "seq")
    return jax.shard_map(local, mesh=mesh, in_specs=in_specs, out_specs=out_specs, check_vma=False)
```

```python
import functools
import math

import jax
import jax.numpy as jnp
from jax import lax
from jax.experimental import pallas as pl
from jax.experimental.pallas import tpu as pltpu
from jax.sharding import PartitionSpec as P

HQ = 64
KVH = 8
HD = 128
NB = 8
QT = 64
GS = 8
ROWS = GS * QT
TILE = 256
MASKED = -1e30
EXP2_SCALE = math.log2(math.e) / math.sqrt(HD)
F32 = jnp.float32
BF16 = jnp.bfloat16
MESH = pl.DeviceIdType.MESH
Q0, Q1, Q2, Q3, C1, C1M, C3, C3M, C4 = range(9)


def kernel(
    heads_ref, len_ref, q_hbm, kv_hbm, w_hbm, out_ref,
    qown, q0recv, cand, q1recv, qall, kv, w, s0, s1, p0, p1, m0, m1,
    osend, mlbuf, c1recv, c1ml, c3send, c3sml, c3recv, c3ml, attall,
    ysend, yown, d1recv, d2send, d2recv, ssem, rsem, dssem, drsem, lsem,
):
    s = lax.axis_index("seq")
    t = lax.axis_index("tp")
    z = t // 2
    c = t % 2
    other = 1 - c
    length = kv.shape[1]
    head = heads_ref[s]
    head_chip = head // 2
    head_core = head % 2

    def slot_of(h):
        slot = jnp.int32(0)
        for k in range(KVH):
            slot = jnp.where(heads_ref[k] == h, k, slot)
        return slot

    slots = [slot_of(k) for k in range(KVH)]
    partner = {"tp": t + 1 - 2 * c}

    def zpeer(d):
        zz = (z + d) % 4
        return zz, {"tp": 2 * zz + c}

    def send(src, dst, ss, rs, dev):
        pltpu.make_async_remote_copy(
            src_ref=src, dst_ref=dst, send_sem=ss, recv_sem=rs, device_id=dev, device_id_type=MESH
        ).start()

    def got(ref, rs):
        pltpu.make_async_remote_copy(
            src_ref=ref, dst_ref=ref, send_sem=rs, recv_sem=rs, device_id=partner, device_id_type=MESH
        ).wait_recv()

    def sent(ref, ss):
        pltpu.make_async_remote_copy(
            src_ref=ref, dst_ref=ref, send_sem=ss, recv_sem=ss, device_id=partner, device_id_type=MESH
        ).wait_send()

    barrier = pltpu.get_barrier_semaphore()
    for d in range(1, 8):
        pl.semaphore_signal(barrier, inc=1, device_id={"tp": (t + d) % 8}, device_id_type=MESH)
        pl.semaphore_signal(barrier, inc=1, device_id={"seq": (s + d) % 8}, device_id_type=MESH)

    qload = pltpu.make_async_copy(q_hbm, qown, lsem.at[NB])
    qload.start()

    def kv_load(b):
        return pltpu.make_async_copy(kv_hbm.at[b], kv.at[b], lsem.at[b])

    wload = pltpu.make_async_copy(w_hbm, w, lsem.at[NB + 1])
    qload.wait()
    for b in range(NB):
        kv_load(b).start()
    wload.start()
    pl.semaphore_wait(barrier, 14)

    half = pl.multiple_of(c * 512, 512)
    other_half = pl.multiple_of(other * 512, 512)
    for b in range(NB):
        send(qown.at[b, :, pl.ds(other_half, 512)], q0recv.at[b], ssem.at[Q0, b], rsem.at[Q0, b], partner)

    def q1(b):
        got(q0recv.at[b], rsem.at[Q0, b])
        mine = qown[b, :, pl.ds(half, 512)]
        x = jnp.where(head_core == c, mine, q0recv[b])
        for k in range(4):
            cand[b, k] = x[:, k * HD : (k + 1) * HD]
        q1recv[b, z] = cand[b, z]
        for d in (2, 1, 3):
            zz, dev = zpeer(d)
            send(cand.at[b, zz], q1recv.at[b, z], ssem.at[Q1, b], rsem.at[Q1, b], dev)

    def q2(b):
        got(q1recv.at[b, pl.ds(0, 3)], rsem.at[Q1, b])
        qall[b, 4 * c + z] = pick([q1recv[b, k] for k in range(4)], head_chip)
        for d in (2, 1, 3):
            _, dev = zpeer(d)
            piece = qall.at[b, 4 * c + z]
            send(piece, piece, ssem.at[Q2, b], rsem.at[Q2, b], dev)

    def q3(b):
        got(q1recv.at[b, pl.ds(0, 3)], rsem.at[Q2, b])
        piece = qall.at[b, pl.ds(4 * c, 4)]
        send(piece, piece, ssem.at[Q3, b], rsem.at[Q3, b], partner)

    def q4(b):
        got(qall.at[b, pl.ds(4 * other, 4)], rsem.at[Q3, b])

    def pick(pieces, index):
        x = pieces[0]
        for k in range(1, len(pieces)):
            x = jnp.where(index == k, pieces[k], x)
        return x

    S, PR, M = (s0, s1), (p0, p1), (m0, m1)
    first = (4 * c, 4 * other)
    row_of = lax.broadcasted_iota(jnp.int32, (TILE, HD), 0)
    lane_of = lax.broadcasted_iota(jnp.int32, (TILE, HD), 1)
    hot = jnp.where(row_of % QT == lane_of, 1.0, 0.0).astype(BF16)
    ahead = (row_of[:HD] - lane_of[:HD]).astype(F32).astype(BF16)
    row, lane = row_of[:QT], lane_of[:QT]

    def bias(start, k):
        edge = jnp.clip(start - HD * k, -200, 200).astype(F32)
        edge = jnp.full((HD, HD), edge, F32).astype(BF16)
        return jnp.where(ahead > edge, jnp.asarray(MASKED, BF16), jnp.asarray(0, BF16))

    def qk(b, r):
        start = len_ref[b] - QT - t * length
        q = jnp.concatenate([qall[b, pl.ds(first[r], 4)].reshape(TILE, HD), hot], axis=1)
        top = None
        for k in range(length // 512):
            extra = jnp.concatenate([bias(start, 4 * k + i) for i in range(4)], axis=0)
            keys = jnp.concatenate([kv[b, k * 512 : (k + 1) * 512, :HD], extra], axis=1)
            x = lax.dot_general(q, keys, (((1,), (1,)), ((), ())), preferred_element_type=F32)
            S[r][:, k * 512 : (k + 1) * 512] = x
            for j in range(4):
                part = x[:, j * HD : (j + 1) * HD]
                top = part if top is None else jnp.maximum(top, part)
        M[r][...] = jnp.broadcast_to(jnp.max(top, axis=1, keepdims=True), (TILE, HD))

    def weigh(r):
        m = M[r][...]
        for k in range(length // HD):
            x = S[r][:, k * HD : (k + 1) * HD]
            PR[r][:, k * HD : (k + 1) * HD] = jnp.exp2((x - m) * EXP2_SCALE).astype(BF16)

    def pv(b, r):
        vals = jnp.concatenate([kv[b, :, HD:], jnp.ones((length, HD), BF16)], axis=1)
        acc = jnp.dot(PR[r][...], vals, preferred_element_type=F32)
        m = M[r][...]
        osend[b, pl.ds(first[r], 4)] = acc[:, :HD].astype(BF16).reshape(4, QT, HD)
        for j in range(4):
            rows = slice(j * QT, (j + 1) * QT)
            x = jnp.where(lane == row, m[rows], 0.0) + jnp.where(lane == row + QT, acc[rows, HD:], 0.0)
            mlbuf[b, first[r] + j] = jnp.sum(x, axis=0, keepdims=True)

    def to_rows(x):
        return jnp.sum(jnp.where(lane == row, jnp.broadcast_to(x, (QT, HD)), 0.0), axis=1, keepdims=True)

    def c1(b):
        c1recv[b, s] = osend[b, s]
        c1ml[b, s] = mlbuf[b, s]
        for d in (6, 2, 3, 5, 7, 1, 4):
            ss = (s + d) % 8
            send(osend.at[b, ss], c1recv.at[b, s], ssem.at[C1, b], rsem.at[C1, b], {"seq": ss})
            send(mlbuf.at[b, ss], c1ml.at[b, s], ssem.at[C1M, b], rsem.at[C1M, b], {"seq": ss})

    def c3(b):
        got(c1recv.at[b, pl.ds(0, 7)], rsem.at[C1, b])
        got(c1ml.at[b, pl.ds(0, 7)], rsem.at[C1M, b])
        pieces = [c1recv[b, k] for k in range(KVH)]
        rows = [c1ml[b, k] for k in range(KVH)]
        for k in range(KVH):
            c3send[b, k] = pick(pieces, slots[k])
            c3sml[b, k] = pick(rows, slots[k])
        c3recv[b, t] = c3send[b, t]
        c3ml[b, t] = c3sml[b, t]
        for d in (4, 5, 3, 2, 6, 7, 1):
            tt = (t + d) % 8
            send(c3send.at[b, tt], c3recv.at[b, t], ssem.at[C3, b], rsem.at[C3, b], {"tp": tt})
            send(c3sml.at[b, tt], c3ml.at[b, t], ssem.at[C3M, b], rsem.at[C3M, b], {"tp": tt})

    def c4(b):
        got(c3recv.at[b, pl.ds(0, 7)], rsem.at[C3, b])
        got(c3ml.at[b, pl.ds(0, 7)], rsem.at[C3M, b])
        ml = c3ml[b].reshape(8, HD)
        top = jnp.max(ml, axis=0, keepdims=True)
        scale = jnp.exp2((ml - top) * EXP2_SCALE)
        total = jnp.sum(ml * pltpu.roll(scale, QT, 1), axis=0, keepdims=True)
        scale = scale / pltpu.roll(jnp.broadcast_to(total, (8, HD)), QT, 1)
        x = c3recv[b, 0].astype(F32) * to_rows(scale[:1])
        for k in range(1, 8):
            x = x + c3recv[b, k].astype(F32) * to_rows(scale[k : k + 1])
        attall[b, s] = x.astype(BF16)
        for d in (6, 2, 3, 5, 7, 1, 4):
            piece = attall.at[b, s]
            send(piece, piece, ssem.at[C4, b], rsem.at[C4, b], {"seq": (s + d) % 8})

    def c5(b):
        got(c1recv.at[b, pl.ds(0, 7)], rsem.at[C4, b])
        x = jnp.concatenate([attall[b, j] for j in range(GS)], axis=1)
        y = jnp.dot(x, w[...], preferred_element_type=F32)

        @pl.when(c == b % 2)
        def _():
            yown[b // 2] = y

        @pl.when(c != b % 2)
        def _():
            ysend[b // 2] = y.astype(BF16)
            send(ysend.at[b // 2], d1recv.at[b // 2], dssem.at[0, b // 2], drsem.at[0, b // 2], partner)

    def d2(b):
        k = b // 2

        @pl.when(c == b % 2)
        def _():
            got(d1recv.at[k], drsem.at[0, k])
            d2send[k] = (yown[k] + d1recv[k].astype(F32)).astype(BF16)

            @pl.when(z == k)
            def _():
                d2recv[k] = d2send[k]

            @pl.when(z != k)
            def _():
                send(d2send.at[k], d2recv.at[z], dssem.at[1, k], drsem.at[1, 0], {"tp": b})

    for step, b in (
        (q1, 0), (q1, 1), (q1, 2), (q1, 3), (q2, 0), (q1, 4), (q2, 1), (q1, 5), (q2, 2), (q2, 3), (q3, 0),
    ):
        step(b)
    kv_load(0).wait()
    qk(0, 0)
    q3(1)

    def guarded(step, b):
        pl.when((b >= 0) & (b < NB))(lambda: step(b))

    def body(b, carry):
        for step, lead in ((q4, 0), (c1, -1), (q3, 2), (q2, 4), (q1, 6), (c3, -4), (c4, -7)):
            guarded(step, b + lead)
        after = jnp.minimum(b + 1, NB - 1)
        pl.when(b + 1 < NB)(lambda: kv_load(after).wait())
        qk(b, 1)
        weigh(0)
        pv(b, 0)
        weigh(1)
        qk(after, 0)
        pv(b, 1)
        return carry

    lax.fori_loop(0, NB, body, 0)
    c1(7)
    wload.wait()
    for step, b in (
        (c3, 4), (c4, 1), (c4, 2), (c3, 5), (c4, 3), (c3, 6), (c5, 0), (c4, 4), (c5, 1), (c3, 7), (c4, 5), (c5, 2), (d2, 0),
        (c4, 6), (d2, 1), (c5, 3), (c4, 7), (c5, 4), (d2, 2), (d2, 3), (c5, 5), (d2, 4), (c5, 6), (d2, 5), (c5, 7), (d2, 6), (d2, 7),
    ):
        step(b)
    got(d2recv.at[pl.ds(0, 3)], drsem.at[1, 0])
    out_ref[0] = jnp.sum(d2recv[...].astype(F32), axis=0).astype(BF16)

    def drain(b, carry):
        sent(q0recv.at[b], ssem.at[Q0, b])
        sent(q1recv.at[b, pl.ds(0, 3)], ssem.at[Q1, b])
        sent(q1recv.at[b, pl.ds(0, 3)], ssem.at[Q2, b])
        sent(qall.at[b, pl.ds(0, 4)], ssem.at[Q3, b])
        for k in (C1, C3, C4):
            sent(c1recv.at[b, pl.ds(0, 7)], ssem.at[k, b])
        for k in (C1M, C3M):
            sent(c1ml.at[b, pl.ds(0, 7)], ssem.at[k, b])
        return carry

    lax.fori_loop(0, NB, drain, 0)
    for k in range(4):
        sent(d1recv.at[k], dssem.at[0, k])
        pl.when(z != k)(lambda k=k: sent(d2send.at[k], dssem.at[1, k]))


def local(query, cache, head_of_slot, lengths, out_weight):
    length = cache.shape[1]
    entries = cache.reshape(NB, length, 2 * HD)
    wide = out_weight.shape[1]
    vm = pltpu.VMEM
    dma = pltpu.SemaphoreType.DMA
    smem = pl.BlockSpec(memory_space=pltpu.SMEM)
    anywhere = pl.BlockSpec(memory_space=pl.ANY)
    return pl.pallas_call(
        kernel,
        out_shape=jax.ShapeDtypeStruct((1, QT, wide), BF16),
        in_specs=[smem, smem, anywhere, anywhere, anywhere],
        out_specs=pl.BlockSpec(memory_space=pltpu.VMEM),
        scratch_shapes=[
            vm((NB, QT, GS * HD), BF16),
            vm((NB, QT, 4 * HD), BF16),
            vm((NB, 4, QT, HD), BF16),
            vm((NB, 4, QT, HD), BF16),
            vm((NB, GS, QT, HD), BF16),
            vm((NB, length, 2 * HD), BF16),
            vm(out_weight.shape, BF16),
            vm((TILE, length), F32),
            vm((TILE, length), F32),
            vm((TILE, length), BF16),
            vm((TILE, length), BF16),
            vm((TILE, HD), F32),
            vm((TILE, HD), F32),
            vm((NB, GS, QT, HD), BF16),
            vm((NB, GS, 1, HD), F32),
            vm((NB, KVH, QT, HD), BF16),
            vm((NB, KVH, 1, HD), F32),
            vm((NB, KVH, QT, HD), BF16),
            vm((NB, KVH, 1, HD), F32),
            vm((NB, 8, QT, HD), BF16),
            vm((NB, 8, 1, HD), F32),
            vm((NB, GS, QT, HD), BF16),
            vm((4, QT, wide), BF16),
            vm((4, QT, wide), F32),
            vm((4, QT, wide), BF16),
            vm((4, QT, wide), BF16),
            vm((4, QT, wide), BF16),
            dma((9, NB)),
            dma((9, NB)),
            dma((2, 4)),
            dma((2, 4)),
            dma((NB + 2,)),
        ],
        compiler_params=pltpu.CompilerParams(
            collective_id=0, has_side_effects=True, vmem_limit_bytes=40 * 2**20
        ),
        name="attend",
    )(*[pltpu.with_memory_space_constraint(x, pltpu.HBM) for x in (head_of_slot, lengths, query, entries, out_weight)])


def solution(mesh):
    in_specs = (
        P("grp", None, "tp"),
        P("grp", "tp", "seq", None),
        P("grp"),
        P("grp"),
        P("tp", "seq"),
    )
    out_specs = P(("grp", "tp"), None, "seq")
    return jax.shard_map(local, mesh=mesh, in_specs=in_specs, out_specs=out_specs, check_vma=False)
```

```python
import functools
import math

import jax
import jax.numpy as jnp
from jax import lax
from jax.experimental import pallas as pl
from jax.experimental.pallas import tpu as pltpu
from jax.sharding import PartitionSpec as P

HQ = 64
KVH = 8
HD = 128
NB = 8
QT = 64
GS = 8
ROWS = GS * QT
TILE = 256
MASKED = -1e30
EXP2_SCALE = math.log2(math.e) / math.sqrt(HD)
F32 = jnp.float32
BF16 = jnp.bfloat16
MESH = pl.DeviceIdType.MESH
Q0, Q1, Q2, Q3, C1, C1M, C3, C3M, C4 = range(9)


def sequence(i):
    return 2 * ((i + 3) % 4) + (i + i // 4 + 1) % 2


def kernel(
    heads_ref, len_ref, q_hbm, kv_hbm, w_hbm, out_ref,
    qown, q0recv, cand, q1recv, qall, kv, w, s0, s1, p0, p1, m0, m1,
    osend, mlbuf, c1recv, c1ml, c3send, c3sml, c3recv, c3ml, attall,
    ysend, yown, d1recv, d2send, d2recv, ssem, rsem, dssem, drsem, lsem,
):
    s = lax.axis_index("seq")
    t = lax.axis_index("tp")
    z = t // 2
    c = t % 2
    other = 1 - c
    length = kv.shape[1]
    head = heads_ref[s]
    head_chip = head // 2
    head_core = head % 2

    def slot_of(h):
        slot = jnp.int32(0)
        for k in range(KVH):
            slot = jnp.where(heads_ref[k] == h, k, slot)
        return slot

    slots = [slot_of(k) for k in range(KVH)]
    partner = {"tp": t + 1 - 2 * c}

    def zpeer(d):
        zz = (z + d) % 4
        return zz, {"tp": 2 * zz + c}

    def send(src, dst, ss, rs, dev):
        pltpu.make_async_remote_copy(
            src_ref=src, dst_ref=dst, send_sem=ss, recv_sem=rs, device_id=dev, device_id_type=MESH
        ).start()

    def got(ref, rs):
        pltpu.make_async_remote_copy(
            src_ref=ref, dst_ref=ref, send_sem=rs, recv_sem=rs, device_id=partner, device_id_type=MESH
        ).wait_recv()

    def sent(ref, ss):
        pltpu.make_async_remote_copy(
            src_ref=ref, dst_ref=ref, send_sem=ss, recv_sem=ss, device_id=partner, device_id_type=MESH
        ).wait_send()

    barrier = pltpu.get_barrier_semaphore()
    for d in range(1, 8):
        pl.semaphore_signal(barrier, inc=1, device_id={"tp": (t + d) % 8}, device_id_type=MESH)
        pl.semaphore_signal(barrier, inc=1, device_id={"seq": (s + d) % 8}, device_id_type=MESH)

    qload = pltpu.make_async_copy(q_hbm, qown, lsem.at[NB])
    qload.start()

    def kv_load(b):
        return pltpu.make_async_copy(kv_hbm.at[sequence(b)], kv.at[b], lsem.at[b])

    wload = pltpu.make_async_copy(w_hbm, w, lsem.at[NB + 1])
    qload.wait()
    for b in range(NB):
        kv_load(b).start()
    wload.start()
    pl.semaphore_wait(barrier, 14)

    half = pl.multiple_of(c * 512, 512)
    other_half = pl.multiple_of(other * 512, 512)
    for b in range(NB):
        send(qown.at[sequence(b), :, pl.ds(other_half, 512)], q0recv.at[b], ssem.at[Q0, b], rsem.at[Q0, b], partner)

    def q1(b):
        got(q0recv.at[b], rsem.at[Q0, b])
        mine = qown[sequence(b), :, pl.ds(half, 512)]
        x = jnp.where(head_core == c, mine, q0recv[b])
        for k in range(4):
            cand[b, k] = x[:, k * HD : (k + 1) * HD]
        q1recv[b, z] = cand[b, z]
        for d in (2, 1, 3):
            zz, dev = zpeer(d)
            send(cand.at[b, zz], q1recv.at[b, z], ssem.at[Q1, b], rsem.at[Q1, b], dev)

    def q2(b):
        got(q1recv.at[b, pl.ds(0, 3)], rsem.at[Q1, b])
        qall[b, 4 * c + z] = pick([q1recv[b, k] for k in range(4)], head_chip)
        for d in (2, 1, 3):
            _, dev = zpeer(d)
            piece = qall.at[b, 4 * c + z]
            send(piece, piece, ssem.at[Q2, b], rsem.at[Q2, b], dev)

    def q3(b):
        got(q1recv.at[b, pl.ds(0, 3)], rsem.at[Q2, b])
        piece = qall.at[b, pl.ds(4 * c, 4)]
        send(piece, piece, ssem.at[Q3, b], rsem.at[Q3, b], partner)

    def q4(b):
        got(qall.at[b, pl.ds(4 * other, 4)], rsem.at[Q3, b])

    def pick(pieces, index):
        x = pieces[0]
        for k in range(1, len(pieces)):
            x = jnp.where(index == k, pieces[k], x)
        return x

    S, PR, M = (s0, s1), (p0, p1), (m0, m1)
    first = (4 * c, 4 * other)
    row_of = lax.broadcasted_iota(jnp.int32, (TILE, HD), 0)
    lane_of = lax.broadcasted_iota(jnp.int32, (TILE, HD), 1)
    hot = jnp.where(row_of % QT == lane_of, 1.0, 0.0).astype(BF16)
    ahead = (row_of[:HD] - lane_of[:HD]).astype(F32).astype(BF16)
    row, lane = row_of[:QT], lane_of[:QT]

    def bias(start, k):
        edge = jnp.clip(start - HD * k, -200, 200).astype(F32)
        edge = jnp.full((HD, HD), edge, F32).astype(BF16)
        return jnp.where(ahead > edge, jnp.asarray(MASKED, BF16), jnp.asarray(0, BF16))

    def qk(b, r):
        start = len_ref[sequence(b)] - QT - t * length
        q = jnp.concatenate([qall[b, pl.ds(first[r], 4)].reshape(TILE, HD), hot], axis=1)
        top = None
        for k in range(length // 512):
            extra = jnp.concatenate([bias(start, 4 * k + i) for i in range(4)], axis=0)
            keys = jnp.concatenate([kv[b, k * 512 : (k + 1) * 512, :HD], extra], axis=1)
            x = lax.dot_general(q, keys, (((1,), (1,)), ((), ())), preferred_element_type=F32)
            S[r][:, k * 512 : (k + 1) * 512] = x
            for j in range(4):
                part = x[:, j * HD : (j + 1) * HD]
                top = part if top is None else jnp.maximum(top, part)
        M[r][...] = jnp.broadcast_to(jnp.max(top, axis=1, keepdims=True), (TILE, HD))

    def weigh(r):
        m = M[r][...]
        for k in range(length // HD):
            x = S[r][:, k * HD : (k + 1) * HD]
            PR[r][:, k * HD : (k + 1) * HD] = jnp.exp2((x - m) * EXP2_SCALE).astype(BF16)

    def pv(b, r):
        vals = jnp.concatenate([kv[b, :, HD:], jnp.ones((length, HD), BF16)], axis=1)
        acc = jnp.dot(PR[r][...], vals, preferred_element_type=F32)
        m = M[r][...]
        osend[b, pl.ds(first[r], 4)] = acc[:, :HD].astype(BF16).reshape(4, QT, HD)
        for j in range(4):
            rows = slice(j * QT, (j + 1) * QT)
            x = jnp.where(lane == row, m[rows], 0.0) + jnp.where(lane == row + QT, acc[rows, HD:], 0.0)
            mlbuf[b, first[r] + j] = jnp.sum(x, axis=0, keepdims=True)

    def to_rows(x):
        return jnp.sum(jnp.where(lane == row, jnp.broadcast_to(x, (QT, HD)), 0.0), axis=1, keepdims=True)

    def c1(b):
        c1recv[b, s] = osend[b, s]
        c1ml[b, s] = mlbuf[b, s]
        for d in (6, 2, 3, 5, 7, 1, 4):
            ss = (s + d) % 8
            send(osend.at[b, ss], c1recv.at[b, s], ssem.at[C1, b], rsem.at[C1, b], {"seq": ss})
            send(mlbuf.at[b, ss], c1ml.at[b, s], ssem.at[C1M, b], rsem.at[C1M, b], {"seq": ss})

    def c3(b):
        got(c1recv.at[b, pl.ds(0, 7)], rsem.at[C1, b])
        got(c1ml.at[b, pl.ds(0, 7)], rsem.at[C1M, b])
        pieces = [c1recv[b, k] for k in range(KVH)]
        rows = [c1ml[b, k] for k in range(KVH)]
        for k in range(KVH):
            c3send[b, k] = pick(pieces, slots[k])
            c3sml[b, k] = pick(rows, slots[k])
        c3recv[b, t] = c3send[b, t]
        c3ml[b, t] = c3sml[b, t]
        for d in (4, 5, 3, 2, 6, 7, 1):
            tt = (t + d) % 8
            send(c3send.at[b, tt], c3recv.at[b, t], ssem.at[C3, b], rsem.at[C3, b], {"tp": tt})
            send(c3sml.at[b, tt], c3ml.at[b, t], ssem.at[C3M, b], rsem.at[C3M, b], {"tp": tt})

    def c4(b):
        got(c3recv.at[b, pl.ds(0, 7)], rsem.at[C3, b])
        got(c3ml.at[b, pl.ds(0, 7)], rsem.at[C3M, b])
        ml = c3ml[b].reshape(8, HD)
        top = jnp.max(ml, axis=0, keepdims=True)
        scale = jnp.exp2((ml - top) * EXP2_SCALE)
        total = jnp.sum(ml * pltpu.roll(scale, QT, 1), axis=0, keepdims=True)
        scale = scale / pltpu.roll(jnp.broadcast_to(total, (8, HD)), QT, 1)
        x = c3recv[b, 0].astype(F32) * to_rows(scale[:1])
        for k in range(1, 8):
            x = x + c3recv[b, k].astype(F32) * to_rows(scale[k : k + 1])
        attall[b, s] = x.astype(BF16)
        for d in (6, 2, 3, 5, 7, 1, 4):
            piece = attall.at[b, s]
            send(piece, piece, ssem.at[C4, b], rsem.at[C4, b], {"seq": (s + d) % 8})

    def c5(b):
        got(c1recv.at[b, pl.ds(0, 7)], rsem.at[C4, b])
        x = jnp.concatenate([attall[b, j] for j in range(GS)], axis=1)
        y = jnp.dot(x, w[...], preferred_element_type=F32)

        k, core = divmod(sequence(b), 2)

        @pl.when(c == core)
        def _():
            yown[k] = y

        @pl.when(c != core)
        def _():
            ysend[k] = y.astype(BF16)
            send(ysend.at[k], d1recv.at[k], dssem.at[0, k], drsem.at[0, k], partner)

    def d2(b):
        k, core = divmod(sequence(b), 2)

        @pl.when(c == core)
        def _():
            got(d1recv.at[k], drsem.at[0, k])
            d2send[k] = (yown[k] + d1recv[k].astype(F32)).astype(BF16)

            @pl.when(z == k)
            def _():
                d2recv[k] = d2send[k]

            @pl.when(z != k)
            def _():
                send(d2send.at[k], d2recv.at[z], dssem.at[1, k], drsem.at[1, 0], {"tp": sequence(b)})

    for step, b in (
        (q1, 0), (q1, 1), (q1, 2), (q1, 3), (q2, 0), (q2, 1), (q1, 4), (q2, 2), (q1, 5), (q3, 0),
    ):
        step(b)
    kv_load(0).wait()
    qk(0, 0)
    q2(3)

    def guarded(step, b):
        pl.when((b >= 0) & (b < NB))(lambda: step(b))

    def body(b, carry):
        for step, lead in ((q4, 0), (c1, -1), (q3, 1), (q2, 4), (q1, 6), (c3, -4), (c4, -7)):
            guarded(step, b + lead)
        after = jnp.minimum(b + 1, NB - 1)
        pl.when(b + 1 < NB)(lambda: kv_load(after).wait())
        qk(b, 1)
        weigh(0)
        pv(b, 0)
        weigh(1)
        qk(after, 0)
        pv(b, 1)
        return carry

    lax.fori_loop(0, NB, body, 0)
    c1(7)
    wload.wait()
    for step, b in (
        (c3, 4), (c4, 1), (c4, 2), (c3, 5), (c3, 6), (c4, 3), (c3, 7), (c5, 0), (c4, 4), (c5, 1), (c4, 5), (c5, 2), (c4, 6),
        (d2, 0), (c5, 3), (d2, 1), (c4, 7), (c5, 4), (d2, 2), (c5, 5), (d2, 3), (c5, 6), (d2, 4), (d2, 5), (c5, 7), (d2, 6), (d2, 7),
    ):
        step(b)
    got(d2recv.at[pl.ds(0, 3)], drsem.at[1, 0])
    out_ref[0] = jnp.sum(d2recv[...].astype(F32), axis=0).astype(BF16)

    def drain(b, carry):
        sent(q0recv.at[b], ssem.at[Q0, b])
        sent(q1recv.at[b, pl.ds(0, 3)], ssem.at[Q1, b])
        sent(q1recv.at[b, pl.ds(0, 3)], ssem.at[Q2, b])
        sent(qall.at[b, pl.ds(0, 4)], ssem.at[Q3, b])
        for k in (C1, C3, C4):
            sent(c1recv.at[b, pl.ds(0, 7)], ssem.at[k, b])
        for k in (C1M, C3M):
            sent(c1ml.at[b, pl.ds(0, 7)], ssem.at[k, b])
        return carry

    lax.fori_loop(0, NB, drain, 0)
    for k in range(4):
        sent(d1recv.at[k], dssem.at[0, k])
        pl.when(z != k)(lambda k=k: sent(d2send.at[k], dssem.at[1, k]))


def local(query, cache, head_of_slot, lengths, out_weight):
    length = cache.shape[1]
    entries = cache.reshape(NB, length, 2 * HD)
    wide = out_weight.shape[1]
    vm = pltpu.VMEM
    dma = pltpu.SemaphoreType.DMA
    smem = pl.BlockSpec(memory_space=pltpu.SMEM)
    anywhere = pl.BlockSpec(memory_space=pl.ANY)
    return pl.pallas_call(
        kernel,
        out_shape=jax.ShapeDtypeStruct((1, QT, wide), BF16),
        in_specs=[smem, smem, anywhere, anywhere, anywhere],
        out_specs=pl.BlockSpec(memory_space=pltpu.VMEM),
        scratch_shapes=[
            vm((NB, QT, GS * HD), BF16),
            vm((NB, QT, 4 * HD), BF16),
            vm((NB, 4, QT, HD), BF16),
            vm((NB, 4, QT, HD), BF16),
            vm((NB, GS, QT, HD), BF16),
            vm((NB, length, 2 * HD), BF16),
            vm(out_weight.shape, BF16),
            vm((TILE, length), F32),
            vm((TILE, length), F32),
            vm((TILE, length), BF16),
            vm((TILE, length), BF16),
            vm((TILE, HD), F32),
            vm((TILE, HD), F32),
            vm((NB, GS, QT, HD), BF16),
            vm((NB, GS, 1, HD), F32),
            vm((NB, KVH, QT, HD), BF16),
            vm((NB, KVH, 1, HD), F32),
            vm((NB, KVH, QT, HD), BF16),
            vm((NB, KVH, 1, HD), F32),
            vm((NB, 8, QT, HD), BF16),
            vm((NB, 8, 1, HD), F32),
            vm((NB, GS, QT, HD), BF16),
            vm((4, QT, wide), BF16),
            vm((4, QT, wide), F32),
            vm((4, QT, wide), BF16),
            vm((4, QT, wide), BF16),
            vm((4, QT, wide), BF16),
            dma((9, NB)),
            dma((9, NB)),
            dma((2, 4)),
            dma((2, 4)),
            dma((NB + 2,)),
        ],
        compiler_params=pltpu.CompilerParams(
            collective_id=0, has_side_effects=True, vmem_limit_bytes=40 * 2**20
        ),
        name="attend",
    )(*[pltpu.with_memory_space_constraint(x, pltpu.HBM) for x in (head_of_slot, lengths, query, entries, out_weight)])


def solution(mesh):
    in_specs = (
        P("grp", None, "tp"),
        P("grp", "tp", "seq", None),
        P("grp"),
        P("grp"),
        P("tp", "seq"),
    )
    out_specs = P(("grp", "tp"), None, "seq")
    return jax.shard_map(local, mesh=mesh, in_specs=in_specs, out_specs=out_specs, check_vma=False)
```

```python
import functools
import math

import jax
import jax.numpy as jnp
from jax import lax
from jax.experimental import pallas as pl
from jax.experimental.pallas import tpu as pltpu
from jax.sharding import PartitionSpec as P

HQ = 64
KVH = 8
HD = 128
NB = 8
QT = 64
GS = 8
ROWS = GS * QT
TILE = 256
MASKED = -1e30
EXP2_SCALE = math.log2(math.e) / math.sqrt(HD)
F32 = jnp.float32
BF16 = jnp.bfloat16
MESH = pl.DeviceIdType.MESH
Q0, Q1, Q2, Q3, C1, C1M, C3, C3M, C4 = range(9)


def sequence(i):
    return 2 * ((i + 3) % 4) + (i + i // 4 + 1) % 2


def kernel(
    heads_hbm, len_hbm, q_hbm, kv_hbm, w_hbm, out_ref,
    heads_ref, len_ref, qown, q0recv, cand, q1recv, qall, kv, w, s0, s1, p0, p1, m0, m1,
    osend, mlbuf, c1recv, c1ml, c3send, c3sml, c3recv, c3ml, attall,
    ysend, yown, d1recv, d2send, d2recv, ssem, rsem, dssem, drsem, lsem,
):
    s = lax.axis_index("seq")
    t = lax.axis_index("tp")
    z = t // 2
    c = t % 2
    other = 1 - c
    length = kv.shape[1]
    partner = {"tp": t + 1 - 2 * c}

    def zpeer(d):
        zz = (z + d) % 4
        return zz, {"tp": 2 * zz + c}

    def send(src, dst, ss, rs, dev):
        pltpu.make_async_remote_copy(
            src_ref=src, dst_ref=dst, send_sem=ss, recv_sem=rs, device_id=dev, device_id_type=MESH
        ).start()

    def got(ref, rs):
        pltpu.make_async_remote_copy(
            src_ref=ref, dst_ref=ref, send_sem=rs, recv_sem=rs, device_id=partner, device_id_type=MESH
        ).wait_recv()

    def sent(ref, ss):
        pltpu.make_async_remote_copy(
            src_ref=ref, dst_ref=ref, send_sem=ss, recv_sem=ss, device_id=partner, device_id_type=MESH
        ).wait_send()

    barrier = pltpu.get_barrier_semaphore()
    for d in range(1, 8):
        pl.semaphore_signal(barrier, inc=1, device_id={"tp": (t + d) % 8}, device_id_type=MESH)
        pl.semaphore_signal(barrier, inc=1, device_id={"seq": (s + d) % 8}, device_id_type=MESH)

    qload = pltpu.make_async_copy(q_hbm, qown, lsem.at[NB])
    qload.start()

    def kv_load(b):
        return pltpu.make_async_copy(kv_hbm.at[sequence(b)], kv.at[b], lsem.at[b])

    wload = pltpu.make_async_copy(w_hbm, w, lsem.at[NB + 1])
    heads_load = pltpu.make_async_copy(heads_hbm, heads_ref, lsem.at[NB + 2])
    len_load = pltpu.make_async_copy(len_hbm, len_ref, lsem.at[NB + 3])
    heads_load.start()
    len_load.start()
    heads_load.wait()
    len_load.wait()
    head = heads_ref[s]
    head_chip = head // 2
    head_core = head % 2

    def slot_of(h):
        slot = jnp.int32(0)
        for k in range(KVH):
            slot = jnp.where(heads_ref[k] == h, k, slot)
        return slot

    slots = [slot_of(k) for k in range(KVH)]
    qload.wait()
    for b in range(NB):
        kv_load(b).start()
    wload.start()
    pl.semaphore_wait(barrier, 14)

    half = pl.multiple_of(c * 512, 512)
    other_half = pl.multiple_of(other * 512, 512)
    def q0(b):
        send(qown.at[sequence(b), :, pl.ds(other_half, 512)], q0recv.at[b], ssem.at[Q0, b], rsem.at[Q0, b], partner)

    def q1(b):
        got(q0recv.at[b], rsem.at[Q0, b])
        mine = qown[sequence(b), :, pl.ds(half, 512)]
        x = jnp.where(head_core == c, mine, q0recv[b])
        for k in range(4):
            cand[b, k] = x[:, k * HD : (k + 1) * HD]
        q1recv[b, z] = cand[b, z]
        for d in (2, 1, 3):
            zz, dev = zpeer(d)
            send(cand.at[b, zz], q1recv.at[b, z], ssem.at[Q1, b], rsem.at[Q1, b], dev)

    def q2(b):
        got(q1recv.at[b, pl.ds(0, 3)], rsem.at[Q1, b])
        qall[b, 4 * c + z] = pick([q1recv[b, k] for k in range(4)], head_chip)
        for d in (2, 1, 3):
            _, dev = zpeer(d)
            piece = qall.at[b, 4 * c + z]
            send(piece, piece, ssem.at[Q2, b], rsem.at[Q2, b], dev)

    def q3(b):
        got(q1recv.at[b, pl.ds(0, 3)], rsem.at[Q2, b])
        piece = qall.at[b, pl.ds(4 * c, 4)]
        send(piece, piece, ssem.at[Q3, b], rsem.at[Q3, b], partner)

    def q4(b):
        got(qall.at[b, pl.ds(4 * other, 4)], rsem.at[Q3, b])

    def pick(pieces, index):
        x = pieces[0]
        for k in range(1, len(pieces)):
            x = jnp.where(index == k, pieces[k], x)
        return x

    S, PR, M = (s0, s1), (p0, p1), (m0, m1)
    first = (4 * c, 4 * other)
    row_of = lax.broadcasted_iota(jnp.int32, (TILE, HD), 0)
    lane_of = lax.broadcasted_iota(jnp.int32, (TILE, HD), 1)
    hot = jnp.where(row_of % QT == lane_of, 1.0, 0.0).astype(BF16)
    ahead = (row_of[:HD] - lane_of[:HD]).astype(F32).astype(BF16)
    row, lane = row_of[:QT], lane_of[:QT]

    def bias(start, k):
        edge = jnp.clip(start - HD * k, -200, 200).astype(F32)
        edge = jnp.full((HD, HD), edge, F32).astype(BF16)
        return jnp.where(ahead > edge, jnp.asarray(MASKED, BF16), jnp.asarray(0, BF16))

    def qk(b, r):
        start = len_ref[sequence(b)] - QT - t * length
        q = jnp.concatenate([qall[b, pl.ds(first[r], 4)].reshape(TILE, HD), hot], axis=1)
        top = None
        for k in range(length // 512):
            extra = jnp.concatenate([bias(start, 4 * k + i) for i in range(4)], axis=0)
            keys = jnp.concatenate([kv[b, k * 512 : (k + 1) * 512, :HD], extra], axis=1)
            x = lax.dot_general(q, keys, (((1,), (1,)), ((), ())), preferred_element_type=F32)
            S[r][:, k * 512 : (k + 1) * 512] = x
            for j in range(4):
                part = x[:, j * HD : (j + 1) * HD]
                top = part if top is None else jnp.maximum(top, part)
        M[r][...] = jnp.broadcast_to(jnp.max(top, axis=1, keepdims=True), (TILE, HD))

    def weigh(r):
        m = M[r][...]
        for k in range(length // HD):
            x = S[r][:, k * HD : (k + 1) * HD]
            PR[r][:, k * HD : (k + 1) * HD] = jnp.exp2((x - m) * EXP2_SCALE).astype(BF16)

    def pv(b, r):
        vals = jnp.concatenate([kv[b, :, HD:], jnp.ones((length, HD), BF16)], axis=1)
        acc = jnp.dot(PR[r][...], vals, preferred_element_type=F32)
        m = M[r][...]
        osend[b, pl.ds(first[r], 4)] = acc[:, :HD].astype(BF16).reshape(4, QT, HD)
        for j in range(4):
            rows = slice(j * QT, (j + 1) * QT)
            x = jnp.where(lane == row, m[rows], 0.0) + jnp.where(lane == row + QT, acc[rows, HD:], 0.0)
            mlbuf[b, first[r] + j] = jnp.sum(x, axis=0, keepdims=True)

    def to_rows(x):
        return jnp.sum(jnp.where(lane == row, jnp.broadcast_to(x, (QT, HD)), 0.0), axis=1, keepdims=True)

    def c1(b):
        c1recv[b, s] = osend[b, s]
        c1ml[b, s] = mlbuf[b, s]
        for d in (6, 2, 3, 5, 7, 1, 4):
            ss = (s + d) % 8
            send(osend.at[b, ss], c1recv.at[b, s], ssem.at[C1, b], rsem.at[C1, b], {"seq": ss})
            send(mlbuf.at[b, ss], c1ml.at[b, s], ssem.at[C1M, b], rsem.at[C1M, b], {"seq": ss})

    def c3(b):
        got(c1recv.at[b, pl.ds(0, 7)], rsem.at[C1, b])
        got(c1ml.at[b, pl.ds(0, 7)], rsem.at[C1M, b])
        pieces = [c1recv[b, k] for k in range(KVH)]
        rows = [c1ml[b, k] for k in range(KVH)]
        for k in range(KVH):
            c3send[b, k] = pick(pieces, slots[k])
            c3sml[b, k] = pick(rows, slots[k])
        c3recv[b, t] = c3send[b, t]
        c3ml[b, t] = c3sml[b, t]
        for d in (4, 5, 3, 2, 6, 7, 1):
            tt = (t + d) % 8
            send(c3send.at[b, tt], c3recv.at[b, t], ssem.at[C3, b], rsem.at[C3, b], {"tp": tt})
            send(c3sml.at[b, tt], c3ml.at[b, t], ssem.at[C3M, b], rsem.at[C3M, b], {"tp": tt})

    def c4(b):
        got(c3recv.at[b, pl.ds(0, 7)], rsem.at[C3, b])
        got(c3ml.at[b, pl.ds(0, 7)], rsem.at[C3M, b])
        ml = c3ml[b].reshape(8, HD)
        top = jnp.max(ml, axis=0, keepdims=True)
        scale = jnp.exp2((ml - top) * EXP2_SCALE)
        total = jnp.sum(ml * pltpu.roll(scale, QT, 1), axis=0, keepdims=True)
        scale = scale / pltpu.roll(jnp.broadcast_to(total, (8, HD)), QT, 1)
        x = c3recv[b, 0].astype(F32) * to_rows(scale[:1])
        for k in range(1, 8):
            x = x + c3recv[b, k].astype(F32) * to_rows(scale[k : k + 1])
        attall[b, s] = x.astype(BF16)
        for d in (6, 2, 3, 5, 7, 1, 4):
            piece = attall.at[b, s]
            send(piece, piece, ssem.at[C4, b], rsem.at[C4, b], {"seq": (s + d) % 8})

    def c5(b):
        got(c1recv.at[b, pl.ds(0, 7)], rsem.at[C4, b])
        x = jnp.concatenate([attall[b, j] for j in range(GS)], axis=1)
        y = jnp.dot(x, w[...], preferred_element_type=F32)

        k, core = divmod(sequence(b), 2)

        @pl.when(c == core)
        def _():
            yown[k] = y

        @pl.when(c != core)
        def _():
            ysend[k] = y.astype(BF16)
            send(ysend.at[k], d1recv.at[k], dssem.at[0, k], drsem.at[0, k], partner)

    def d2(b):
        k, core = divmod(sequence(b), 2)

        @pl.when(c == core)
        def _():
            got(d1recv.at[k], drsem.at[0, k])
            d2send[k] = (yown[k] + d1recv[k].astype(F32)).astype(BF16)

            @pl.when(z == k)
            def _():
                d2recv[k] = d2send[k]

            @pl.when(z != k)
            def _():
                send(d2send.at[k], d2recv.at[z], dssem.at[1, k], drsem.at[1, 0], {"tp": sequence(b)})

    q0(0)
    q1(0)
    for b in range(1, 4):
        q0(b)
    q1(1)
    q1(2)
    for b in range(4, NB):
        q0(b)
    q1(3)
    q2(0)
    q2(1)
    q1(4)
    q2(2)
    q1(5)
    q3(0)
    kv_load(0).wait()
    qk(0, 0)

    def guarded(step, b):
        pl.when((b >= 0) & (b < NB))(lambda: step(b))

    def steps_at(b):
        for step, lead in ((q4, 0), (c1, -1), (q3, 1), (q2, 3), (q1, 6), (c3, -4), (c4, -7)):
            if not isinstance(b, int):
                if step is not c4:
                    guarded(step, b + lead)
            elif 0 <= b + lead < NB:
                step(b + lead)

    def body(b, carry):
        steps_at(b)
        kv_load(b + 1).wait()
        qk(b, 1)
        weigh(0)
        pv(b, 0)
        weigh(1)
        qk(b + 1, 0)
        pv(b, 1)
        return carry

    lax.fori_loop(0, NB - 1, body, 0)
    last = NB - 1
    steps_at(last)
    qk(last, 1)
    weigh(0)
    pv(last, 0)
    weigh(1)
    pv(last, 1)
    c1(last)
    wload.wait()
    for step, b in (
        (c3, 4), (c3, 5), (c4, 1), (c4, 2), (c3, 6), (c4, 3), (c3, 7), (c5, 0), (c4, 4), (c5, 1), (c4, 5), (c5, 2), (c4, 6), (d2, 0), (c5, 3), (d2, 1), (c4, 7), (c5, 4), (d2, 2), (c5, 5), (d2, 3), (c5, 6), (d2, 4), (d2, 5), (c5, 7), (d2, 6), (d2, 7),
    ):
        step(b)
    got(d2recv.at[pl.ds(0, 3)], drsem.at[1, 0])
    out_ref[0] = jnp.sum(d2recv[...].astype(F32), axis=0).astype(BF16)

    def drain(b, carry):
        sent(q0recv.at[b], ssem.at[Q0, b])
        sent(q1recv.at[b, pl.ds(0, 3)], ssem.at[Q1, b])
        sent(q1recv.at[b, pl.ds(0, 3)], ssem.at[Q2, b])
        sent(qall.at[b, pl.ds(0, 4)], ssem.at[Q3, b])
        for k in (C1, C3, C4):
            sent(c1recv.at[b, pl.ds(0, 7)], ssem.at[k, b])
        for k in (C1M, C3M):
            sent(c1ml.at[b, pl.ds(0, 7)], ssem.at[k, b])
        return carry

    lax.fori_loop(0, NB, drain, 0)
    for k in range(4):
        sent(d1recv.at[k], dssem.at[0, k])
        pl.when(z != k)(lambda k=k: sent(d2send.at[k], dssem.at[1, k]))


def local(query, cache, head_of_slot, lengths, out_weight):
    length = cache.shape[1]
    entries = cache.reshape(NB, length, 2 * HD)
    wide = out_weight.shape[1]
    vm = pltpu.VMEM
    dma = pltpu.SemaphoreType.DMA
    anywhere = pl.BlockSpec(memory_space=pl.ANY)
    return pl.pallas_call(
        kernel,
        out_shape=jax.ShapeDtypeStruct((1, QT, wide), BF16),
        in_specs=[anywhere] * 5,
        out_specs=pl.BlockSpec(memory_space=pltpu.VMEM),
        scratch_shapes=[
            pltpu.SMEM((KVH,), jnp.int32),
            pltpu.SMEM((NB,), jnp.int32),
            vm((NB, QT, GS * HD), BF16),
            vm((NB, QT, 4 * HD), BF16),
            vm((NB, 4, QT, HD), BF16),
            vm((NB, 4, QT, HD), BF16),
            vm((NB, GS, QT, HD), BF16),
            vm((NB, length, 2 * HD), BF16),
            vm(out_weight.shape, BF16),
            vm((TILE, length), F32),
            vm((TILE, length), F32),
            vm((TILE, length), BF16),
            vm((TILE, length), BF16),
            vm((TILE, HD), F32),
            vm((TILE, HD), F32),
            vm((NB, GS, QT, HD), BF16),
            vm((NB, GS, 1, HD), F32),
            vm((NB, KVH, QT, HD), BF16),
            vm((NB, KVH, 1, HD), F32),
            vm((NB, KVH, QT, HD), BF16),
            vm((NB, KVH, 1, HD), F32),
            vm((NB, 8, QT, HD), BF16),
            vm((NB, 8, 1, HD), F32),
            vm((NB, GS, QT, HD), BF16),
            vm((4, QT, wide), BF16),
            vm((4, QT, wide), F32),
            vm((4, QT, wide), BF16),
            vm((4, QT, wide), BF16),
            vm((4, QT, wide), BF16),
            dma((9, NB)),
            dma((9, NB)),
            dma((2, 4)),
            dma((2, 4)),
            dma((NB + 4,)),
        ],
        compiler_params=pltpu.CompilerParams(
            collective_id=0, has_side_effects=True, vmem_limit_bytes=40 * 2**20
        ),
        name="attend",
    )(*[pltpu.with_memory_space_constraint(x, pltpu.HBM) for x in (head_of_slot, lengths, query, entries, out_weight)])


def solution(mesh):
    in_specs = (
        P("grp", None, "tp"),
        P("grp", "tp", "seq", None),
        P("grp"),
        P("grp"),
        P("tp", "seq"),
    )
    out_specs = P(("grp", "tp"), None, "seq")
    return jax.shard_map(local, mesh=mesh, in_specs=in_specs, out_specs=out_specs, check_vma=False)
```

```python
import functools
import math

import jax
import jax.numpy as jnp
from jax import lax
from jax.experimental import pallas as pl
from jax.experimental.pallas import tpu as pltpu
from jax.sharding import PartitionSpec as P

HQ = 64
KVH = 8
HD = 128
NB = 8
QT = 64
GS = 8
ROWS = GS * QT
TILE = 256
MASKED = -1e30
EXP2_SCALE = math.log2(math.e) / math.sqrt(HD)
F32 = jnp.float32
BF16 = jnp.bfloat16
MESH = pl.DeviceIdType.MESH
Q0, Q1, Q2, Q3, C1, C1M, C3, C3M, C4 = range(9)


def sequence(i):
    return 2 * ((i + 3) % 4) + (i + i // 4 + 1) % 2


def kernel(
    heads_hbm, len_hbm, q_hbm, kv_hbm, w_hbm, out_ref,
    heads_ref, len_ref, qown, q0recv, cand, q1recv, qall, kv, w, s0, s1, p0, p1, m0, m1,
    osend, mlbuf, c1recv, c1ml, c3send, c3sml, c3recv, c3ml, attall,
    ysend, yown, d1recv, d2send, d2recv, ssem, rsem, dssem, drsem, lsem,
):
    s = lax.axis_index("seq")
    t = lax.axis_index("tp")
    z = t // 2
    c = t % 2
    other = 1 - c
    length = kv.shape[1]
    partner = {"tp": t + 1 - 2 * c}

    def zpeer(d):
        zz = (z + d) % 4
        return zz, {"tp": 2 * zz + c}

    def send(src, dst, ss, rs, dev):
        pltpu.make_async_remote_copy(
            src_ref=src, dst_ref=dst, send_sem=ss, recv_sem=rs, device_id=dev, device_id_type=MESH
        ).start()

    def got(ref, rs):
        pltpu.make_async_remote_copy(
            src_ref=ref, dst_ref=ref, send_sem=rs, recv_sem=rs, device_id=partner, device_id_type=MESH
        ).wait_recv()

    def sent(ref, ss):
        pltpu.make_async_remote_copy(
            src_ref=ref, dst_ref=ref, send_sem=ss, recv_sem=ss, device_id=partner, device_id_type=MESH
        ).wait_send()

    barrier = pltpu.get_barrier_semaphore()
    for d in range(1, 8):
        pl.semaphore_signal(barrier, inc=1, device_id={"tp": (t + d) % 8}, device_id_type=MESH)
        pl.semaphore_signal(barrier, inc=1, device_id={"seq": (s + d) % 8}, device_id_type=MESH)

    qload = pltpu.make_async_copy(q_hbm, qown, lsem.at[NB])
    qload.start()

    def kv_load(b):
        return pltpu.make_async_copy(kv_hbm.at[sequence(b)], kv.at[b], lsem.at[b])

    wload = pltpu.make_async_copy(w_hbm, w, lsem.at[NB + 1])
    heads_load = pltpu.make_async_copy(heads_hbm, heads_ref, lsem.at[NB + 2])
    len_load = pltpu.make_async_copy(len_hbm, len_ref, lsem.at[NB + 3])
    heads_load.start()
    len_load.start()
    heads_load.wait()
    len_load.wait()
    head = heads_ref[s]
    head_chip = head // 2
    head_core = head % 2

    def slot_of(h):
        slot = jnp.int32(0)
        for k in range(KVH):
            slot = jnp.where(heads_ref[k] == h, k, slot)
        return slot

    slots = [slot_of(k) for k in range(KVH)]
    qload.wait()
    for b in range(NB):
        kv_load(b).start()
    wload.start()
    pl.semaphore_wait(barrier, 14)

    half = pl.multiple_of(c * 512, 512)
    other_half = pl.multiple_of(other * 512, 512)
    def q0(b):
        send(qown.at[sequence(b), :, pl.ds(other_half, 512)], q0recv.at[b], ssem.at[Q0, b], rsem.at[Q0, b], partner)

    def q1(b):
        got(q0recv.at[b], rsem.at[Q0, b])
        mine = qown[sequence(b), :, pl.ds(half, 512)]
        x = jnp.where(head_core == c, mine, q0recv[b])
        for k in range(4):
            cand[b, k] = x[:, k * HD : (k + 1) * HD]
        q1recv[b, z] = cand[b, z]
        for d in (2, 1, 3):
            zz, dev = zpeer(d)
            send(cand.at[b, zz], q1recv.at[b, z], ssem.at[Q1, b], rsem.at[Q1, b], dev)

    def q2(b):
        got(q1recv.at[b, pl.ds(0, 3)], rsem.at[Q1, b])
        qall[b, 4 * c + z] = pick([q1recv[b, k] for k in range(4)], head_chip)
        for d in (2, 1, 3):
            _, dev = zpeer(d)
            piece = qall.at[b, 4 * c + z]
            send(piece, piece, ssem.at[Q2, b], rsem.at[Q2, b], dev)

    def q3(b):
        got(q1recv.at[b, pl.ds(0, 3)], rsem.at[Q2, b])
        piece = qall.at[b, pl.ds(4 * c, 4)]
        send(piece, piece, ssem.at[Q3, b], rsem.at[Q3, b], partner)

    def q4(b):
        got(qall.at[b, pl.ds(4 * other, 4)], rsem.at[Q3, b])

    def pick(pieces, index):
        x = pieces[0]
        for k in range(1, len(pieces)):
            x = jnp.where(index == k, pieces[k], x)
        return x

    S, PR, M = (s0, s1), (p0, p1), (m0, m1)
    first = (4 * c, 4 * other)
    row_of = lax.broadcasted_iota(jnp.int32, (TILE, HD), 0)
    lane_of = lax.broadcasted_iota(jnp.int32, (TILE, HD), 1)
    hot = jnp.where(row_of % QT == lane_of, 1.0, 0.0).astype(BF16)
    ahead = (row_of[:HD] - lane_of[:HD]).astype(F32).astype(BF16)
    row, lane = row_of[:QT], lane_of[:QT]

    def bias(start, k):
        edge = jnp.clip(start - HD * k, -200, 200).astype(F32)
        edge = jnp.full((HD, HD), edge, F32).astype(BF16)
        return jnp.where(ahead > edge, jnp.asarray(MASKED, BF16), jnp.asarray(0, BF16))

    def qk(b, r):
        start = len_ref[sequence(b)] - QT - t * length
        q = jnp.concatenate([qall[b, pl.ds(first[r], 4)].reshape(TILE, HD), hot], axis=1)
        top = None
        for k in range(length // 512):
            extra = jnp.concatenate([bias(start, 4 * k + i) for i in range(4)], axis=0)
            keys = jnp.concatenate([kv[b, k * 512 : (k + 1) * 512, :HD], extra], axis=1)
            x = lax.dot_general(q, keys, (((1,), (1,)), ((), ())), preferred_element_type=F32)
            S[r][:, k * 512 : (k + 1) * 512] = x
            for j in range(4):
                part = x[:, j * HD : (j + 1) * HD]
                top = part if top is None else jnp.maximum(top, part)
        M[r][...] = jnp.broadcast_to(jnp.max(top, axis=1, keepdims=True), (TILE, HD))

    def weigh(r):
        m = M[r][...]
        for k in range(length // HD):
            x = S[r][:, k * HD : (k + 1) * HD]
            PR[r][:, k * HD : (k + 1) * HD] = jnp.exp2((x - m) * EXP2_SCALE).astype(BF16)

    def pv(b, r):
        vals = jnp.concatenate([kv[b, :, HD:], jnp.ones((length, HD), BF16)], axis=1)
        acc = jnp.dot(PR[r][...], vals, preferred_element_type=F32)
        m = M[r][...]
        osend[b, pl.ds(first[r], 4)] = acc[:, :HD].astype(BF16).reshape(4, QT, HD)
        for j in range(4):
            rows = slice(j * QT, (j + 1) * QT)
            x = jnp.where(lane == row, m[rows], 0.0) + jnp.where(lane == row + QT, acc[rows, HD:], 0.0)
            mlbuf[b, first[r] + j] = jnp.sum(x, axis=0, keepdims=True)

    def c1(b):
        c1recv[b, s] = osend[b, s]
        c1ml[b, s] = mlbuf[b, s]
        for d in (6, 2, 3, 5, 7, 1, 4):
            ss = (s + d) % 8
            send(mlbuf.at[b, ss], c1ml.at[b, s], ssem.at[C1M, b], rsem.at[C1M, b], {"seq": ss})
        for d in (6, 2, 3, 5, 7, 1, 4):
            ss = (s + d) % 8
            send(osend.at[b, ss], c1recv.at[b, s], ssem.at[C1, b], rsem.at[C1, b], {"seq": ss})

    def c3(b):
        got(c1recv.at[b, pl.ds(0, 7)], rsem.at[C1, b])
        got(c1ml.at[b, pl.ds(0, 7)], rsem.at[C1M, b])
        pieces = [c1recv[b, k] for k in range(KVH)]
        rows = [c1ml[b, k] for k in range(KVH)]
        for k in range(KVH):
            c3send[b, k] = pick(pieces, slots[k])
            c3sml[b, k] = pick(rows, slots[k])
        c3recv[b, t] = c3send[b, t]
        c3ml[b, t] = c3sml[b, t]
        for d in (4, 5, 3, 2, 6, 7, 1):
            tt = (t + d) % 8
            send(c3sml.at[b, tt], c3ml.at[b, t], ssem.at[C3M, b], rsem.at[C3M, b], {"tp": tt})
        for d in (4, 5, 3, 2, 6, 7, 1):
            tt = (t + d) % 8
            send(c3send.at[b, tt], c3recv.at[b, t], ssem.at[C3, b], rsem.at[C3, b], {"tp": tt})

    def c4(b):
        got(c3recv.at[b, pl.ds(0, 7)], rsem.at[C3, b])
        got(c3ml.at[b, pl.ds(0, 7)], rsem.at[C3M, b])
        ml = c3ml[b].reshape(8, HD)
        top = jnp.max(ml, axis=0, keepdims=True)
        scale = jnp.exp2((ml - top) * EXP2_SCALE)
        total = jnp.sum(ml * pltpu.roll(scale, QT, 1), axis=0, keepdims=True)
        scale = scale / pltpu.roll(jnp.broadcast_to(total, (8, HD)), QT, 1)
        columns = jnp.transpose(scale)[:QT]
        x = c3recv[b, 0].astype(F32) * columns[:, :1]
        for k in range(1, 8):
            x = x + c3recv[b, k].astype(F32) * columns[:, k : k + 1]
        attall[b, s] = x.astype(BF16)
        for d in (6, 2, 3, 5, 7, 1, 4):
            piece = attall.at[b, s]
            send(piece, piece, ssem.at[C4, b], rsem.at[C4, b], {"seq": (s + d) % 8})

    def c5(b):
        got(c1recv.at[b, pl.ds(0, 7)], rsem.at[C4, b])
        x = jnp.concatenate([attall[b, j] for j in range(GS)], axis=1)
        y = jnp.dot(x, w[...], preferred_element_type=F32)

        k, core = divmod(sequence(b), 2)

        @pl.when(c == core)
        def _():
            yown[k] = y

        @pl.when(c != core)
        def _():
            ysend[k] = y.astype(BF16)
            send(ysend.at[k], d1recv.at[k], dssem.at[0, k], drsem.at[0, k], partner)

    def d2(b):
        k, core = divmod(sequence(b), 2)

        @pl.when(c == core)
        def _():
            got(d1recv.at[k], drsem.at[0, k])
            d2send[k] = (yown[k] + d1recv[k].astype(F32)).astype(BF16)

            @pl.when(z == k)
            def _():
                d2recv[k] = d2send[k]

            @pl.when(z != k)
            def _():
                send(d2send.at[k], d2recv.at[z], dssem.at[1, k], drsem.at[1, 0], {"tp": sequence(b)})

    q0(0)
    q1(0)
    for b in range(1, 4):
        q0(b)
    q1(1)
    q1(2)
    for b in range(4, NB):
        q0(b)
    q1(3)
    q2(0)
    q2(1)
    q1(4)
    q2(2)
    q1(5)
    q3(0)
    kv_load(0).wait()
    qk(0, 0)

    def guarded(step, b):
        pl.when((b >= 0) & (b < NB))(lambda: step(b))

    def steps_at(b):
        for step, lead in ((q4, 0), (c1, -1), (q3, 1), (q2, 3), (q1, 6), (c3, -4), (c4, -7)):
            if not isinstance(b, int):
                if step is not c4:
                    guarded(step, b + lead)
            elif 0 <= b + lead < NB:
                step(b + lead)

    def body(b, carry):
        steps_at(b)
        kv_load(b + 1).wait()
        qk(b, 1)
        weigh(0)
        pv(b, 0)
        weigh(1)
        qk(b + 1, 0)
        pv(b, 1)
        return carry

    lax.fori_loop(0, NB - 1, body, 0)
    last = NB - 1
    steps_at(last)
    qk(last, 1)
    weigh(0)
    pv(last, 0)
    weigh(1)
    pv(last, 1)
    c1(last)
    wload.wait()
    for step, b in (
        (c3, 4), (c3, 5), (c4, 1), (c4, 2), (c3, 6), (c4, 3), (c3, 7), (c5, 0), (c4, 4), (c5, 1), (c4, 5), (c5, 2), (c4, 6), (d2, 0), (c5, 3), (d2, 1), (c4, 7), (c5, 4), (d2, 2), (c5, 5), (d2, 3), (c5, 6), (d2, 4), (d2, 5), (c5, 7), (d2, 6), (d2, 7),
    ):
        step(b)
    got(d2recv.at[pl.ds(0, 3)], drsem.at[1, 0])
    out_ref[0] = jnp.sum(d2recv[...].astype(F32), axis=0).astype(BF16)

    def drain(b, carry):
        sent(q0recv.at[b], ssem.at[Q0, b])
        sent(q1recv.at[b, pl.ds(0, 3)], ssem.at[Q1, b])
        sent(q1recv.at[b, pl.ds(0, 3)], ssem.at[Q2, b])
        sent(qall.at[b, pl.ds(0, 4)], ssem.at[Q3, b])
        for k in (C1, C3, C4):
            sent(c1recv.at[b, pl.ds(0, 7)], ssem.at[k, b])
        for k in (C1M, C3M):
            sent(c1ml.at[b, pl.ds(0, 7)], ssem.at[k, b])
        return carry

    lax.fori_loop(0, NB, drain, 0)
    for k in range(4):
        sent(d1recv.at[k], dssem.at[0, k])
        pl.when(z != k)(lambda k=k: sent(d2send.at[k], dssem.at[1, k]))


def local(query, cache, head_of_slot, lengths, out_weight):
    length = cache.shape[1]
    entries = cache.reshape(NB, length, 2 * HD)
    wide = out_weight.shape[1]
    vm = pltpu.VMEM
    dma = pltpu.SemaphoreType.DMA
    anywhere = pl.BlockSpec(memory_space=pl.ANY)
    return pl.pallas_call(
        kernel,
        out_shape=jax.ShapeDtypeStruct((1, QT, wide), BF16),
        in_specs=[anywhere] * 5,
        out_specs=pl.BlockSpec(memory_space=pltpu.VMEM),
        scratch_shapes=[
            pltpu.SMEM((KVH,), jnp.int32),
            pltpu.SMEM((NB,), jnp.int32),
            vm((NB, QT, GS * HD), BF16),
            vm((NB, QT, 4 * HD), BF16),
            vm((NB, 4, QT, HD), BF16),
            vm((NB, 4, QT, HD), BF16),
            vm((NB, GS, QT, HD), BF16),
            vm((NB, length, 2 * HD), BF16),
            vm(out_weight.shape, BF16),
            vm((TILE, length), F32),
            vm((TILE, length), F32),
            vm((TILE, length), BF16),
            vm((TILE, length), BF16),
            vm((TILE, HD), F32),
            vm((TILE, HD), F32),
            vm((NB, GS, QT, HD), BF16),
            vm((NB, GS, 1, HD), F32),
            vm((NB, KVH, QT, HD), BF16),
            vm((NB, KVH, 1, HD), F32),
            vm((NB, KVH, QT, HD), BF16),
            vm((NB, KVH, 1, HD), F32),
            vm((NB, 8, QT, HD), BF16),
            vm((NB, 8, 1, HD), F32),
            vm((NB, GS, QT, HD), BF16),
            vm((4, QT, wide), BF16),
            vm((4, QT, wide), F32),
            vm((4, QT, wide), BF16),
            vm((4, QT, wide), BF16),
            vm((4, QT, wide), BF16),
            dma((9, NB)),
            dma((9, NB)),
            dma((2, 4)),
            dma((2, 4)),
            dma((NB + 4,)),
        ],
        compiler_params=pltpu.CompilerParams(
            collective_id=0, has_side_effects=True, vmem_limit_bytes=40 * 2**20
        ),
        name="attend",
    )(*[pltpu.with_memory_space_constraint(x, pltpu.HBM) for x in (head_of_slot, lengths, query, entries, out_weight)])


def solution(mesh):
    in_specs = (
        P("grp", None, "tp"),
        P("grp", "tp", "seq", None),
        P("grp"),
        P("grp"),
        P("tp", "seq"),
    )
    out_specs = P(("grp", "tp"), None, "seq")
    return jax.shard_map(local, mesh=mesh, in_specs=in_specs, out_specs=out_specs, check_vma=False)
```

```python
import functools
import math

import jax
import jax.numpy as jnp
from jax import lax
from jax.experimental import pallas as pl
from jax.experimental.pallas import tpu as pltpu
from jax.sharding import PartitionSpec as P

HQ = 64
KVH = 8
HD = 128
NB = 8
QT = 64
GS = 8
ROWS = GS * QT
TILE = 256
MASKED = -1e30
EXP2_SCALE = math.log2(math.e) / math.sqrt(HD)
F32 = jnp.float32
BF16 = jnp.bfloat16
MESH = pl.DeviceIdType.MESH
Q0, Q1, Q2, Q3, C1, C1M, C3, C3M, C4 = range(9)


def sequence(i):
    return 2 * ((i + 3) % 4) + (i + i // 4 + 1) % 2


def kernel(
    heads_hbm, len_hbm, q_hbm, kv_hbm, w_hbm, out_ref,
    heads_ref, len_ref, qown, q0recv, cand, q1recv, qall, kv, w, s0, s1, p0, p1, m0, m1,
    osend, mlbuf, c1recv, c1ml, c3send, c3sml, c3recv, c3ml, attall,
    ysend, yown, d1recv, d2send, d2recv, ssem, rsem, dssem, drsem, lsem,
):
    s = lax.axis_index("seq")
    t = lax.axis_index("tp")
    z = t // 2
    c = t % 2
    other = 1 - c
    length = kv.shape[1]
    partner = {"tp": t + 1 - 2 * c}

    def zpeer(d):
        zz = (z + d) % 4
        return zz, {"tp": 2 * zz + c}

    def send(src, dst, ss, rs, dev):
        pltpu.make_async_remote_copy(
            src_ref=src, dst_ref=dst, send_sem=ss, recv_sem=rs, device_id=dev, device_id_type=MESH
        ).start()

    def got(ref, rs):
        pltpu.make_async_remote_copy(
            src_ref=ref, dst_ref=ref, send_sem=rs, recv_sem=rs, device_id=partner, device_id_type=MESH
        ).wait_recv()

    def sent(ref, ss):
        pltpu.make_async_remote_copy(
            src_ref=ref, dst_ref=ref, send_sem=ss, recv_sem=ss, device_id=partner, device_id_type=MESH
        ).wait_send()

    barrier = pltpu.get_barrier_semaphore()
    for d in range(1, 8):
        pl.semaphore_signal(barrier, inc=1, device_id={"tp": (t + d) % 8}, device_id_type=MESH)
        pl.semaphore_signal(barrier, inc=1, device_id={"seq": (s + d) % 8}, device_id_type=MESH)

    def q_load(b):
        return pltpu.make_async_copy(q_hbm.at[sequence(b)], qown.at[sequence(b)], lsem.at[NB + 4 + b])

    for b in range(NB):
        q_load(b).start()

    def kv_load(b):
        return pltpu.make_async_copy(kv_hbm.at[sequence(b)], kv.at[b], lsem.at[b])

    wload = pltpu.make_async_copy(w_hbm, w, lsem.at[NB + 1])
    heads_load = pltpu.make_async_copy(heads_hbm, heads_ref, lsem.at[NB + 2])
    len_load = pltpu.make_async_copy(len_hbm, len_ref, lsem.at[NB + 3])
    heads_load.start()
    len_load.start()
    heads_load.wait()
    len_load.wait()
    head = heads_ref[s]
    head_chip = head // 2
    head_core = head % 2

    def slot_of(h):
        slot = jnp.int32(0)
        for k in range(KVH):
            slot = jnp.where(heads_ref[k] == h, k, slot)
        return slot

    slots = [slot_of(k) for k in range(KVH)]
    q_load(0).wait()
    for b in range(NB):
        kv_load(b).start()
    wload.start()
    pl.semaphore_wait(barrier, 14)

    half = pl.multiple_of(c * 512, 512)
    other_half = pl.multiple_of(other * 512, 512)
    def q0(b):
        if b:
            q_load(b).wait()
        send(qown.at[sequence(b), :, pl.ds(other_half, 512)], q0recv.at[b], ssem.at[Q0, b], rsem.at[Q0, b], partner)

    def q1(b):
        got(q0recv.at[b], rsem.at[Q0, b])
        mine = qown[sequence(b), :, pl.ds(half, 512)]
        x = jnp.where(head_core == c, mine, q0recv[b])
        for k in range(4):
            cand[b, k] = x[:, k * HD : (k + 1) * HD]
        q1recv[b, z] = cand[b, z]
        for d in (2, 1, 3):
            zz, dev = zpeer(d)
            send(cand.at[b, zz], q1recv.at[b, z], ssem.at[Q1, b], rsem.at[Q1, b], dev)

    def q2(b):
        got(q1recv.at[b, pl.ds(0, 3)], rsem.at[Q1, b])
        qall[b, 4 * c + z] = pick([q1recv[b, k] for k in range(4)], head_chip)
        for d in (2, 1, 3):
            _, dev = zpeer(d)
            piece = qall.at[b, 4 * c + z]
            send(piece, piece, ssem.at[Q2, b], rsem.at[Q2, b], dev)

    def q3(b):
        got(q1recv.at[b, pl.ds(0, 3)], rsem.at[Q2, b])
        piece = qall.at[b, pl.ds(4 * c, 4)]
        send(piece, piece, ssem.at[Q3, b], rsem.at[Q3, b], partner)

    def q4(b):
        got(qall.at[b, pl.ds(4 * other, 4)], rsem.at[Q3, b])

    def pick(pieces, index):
        x = pieces[0]
        for k in range(1, len(pieces)):
            x = jnp.where(index == k, pieces[k], x)
        return x

    S, PR, M = (s0, s1), (p0, p1), (m0, m1)
    first = (4 * c, 4 * other)
    row_of = lax.broadcasted_iota(jnp.int32, (TILE, HD), 0)
    lane_of = lax.broadcasted_iota(jnp.int32, (TILE, HD), 1)
    hot = jnp.where(row_of % QT == lane_of, 1.0, 0.0).astype(BF16)
    ahead = (row_of[:HD] - lane_of[:HD]).astype(F32).astype(BF16)
    row, lane = row_of[:QT], lane_of[:QT]

    def bias(start, k):
        edge = jnp.clip(start - HD * k, -200, 200).astype(F32)
        edge = jnp.full((HD, HD), edge, F32).astype(BF16)
        return jnp.where(ahead > edge, jnp.asarray(MASKED, BF16), jnp.asarray(0, BF16))

    def qk(b, r):
        start = len_ref[sequence(b)] - QT - t * length
        q = jnp.concatenate([qall[b, pl.ds(first[r], 4)].reshape(TILE, HD), hot], axis=1)
        top = None
        for k in range(length // 512):
            extra = jnp.concatenate([bias(start, 4 * k + i) for i in range(4)], axis=0)
            keys = jnp.concatenate([kv[b, k * 512 : (k + 1) * 512, :HD], extra], axis=1)
            x = lax.dot_general(q, keys, (((1,), (1,)), ((), ())), preferred_element_type=F32)
            S[r][:, k * 512 : (k + 1) * 512] = x
            for j in range(4):
                part = x[:, j * HD : (j + 1) * HD]
                top = part if top is None else jnp.maximum(top, part)
        M[r][...] = jnp.broadcast_to(jnp.max(top, axis=1, keepdims=True), (TILE, HD))

    def weigh(r):
        m = M[r][...]
        for k in range(length // HD):
            x = S[r][:, k * HD : (k + 1) * HD]
            PR[r][:, k * HD : (k + 1) * HD] = jnp.exp2((x - m) * EXP2_SCALE).astype(BF16)

    def pv(b, r):
        vals = jnp.concatenate([kv[b, :, HD:], jnp.ones((length, HD), BF16)], axis=1)
        acc = jnp.dot(PR[r][...], vals, preferred_element_type=F32)
        m = M[r][...]
        osend[b, pl.ds(first[r], 4)] = acc[:, :HD].astype(BF16).reshape(4, QT, HD)
        for j in range(4):
            rows = slice(j * QT, (j + 1) * QT)
            x = jnp.where(lane == row, m[rows], 0.0) + jnp.where(lane == row + QT, acc[rows, HD:], 0.0)
            mlbuf[b, first[r] + j] = jnp.sum(x, axis=0, keepdims=True)

    def to_rows(x):
        return jnp.sum(jnp.where(lane == row, jnp.broadcast_to(x, (QT, HD)), 0.0), axis=1, keepdims=True)

    def c1(b):
        c1recv[b, s] = osend[b, s]
        c1ml[b, s] = mlbuf[b, s]
        for d in (6, 2, 3, 5, 7, 1, 4):
            ss = (s + d) % 8
            send(osend.at[b, ss], c1recv.at[b, s], ssem.at[C1, b], rsem.at[C1, b], {"seq": ss})
            send(mlbuf.at[b, ss], c1ml.at[b, s], ssem.at[C1M, b], rsem.at[C1M, b], {"seq": ss})

    def c3(b):
        got(c1recv.at[b, pl.ds(0, 7)], rsem.at[C1, b])
        got(c1ml.at[b, pl.ds(0, 7)], rsem.at[C1M, b])
        pieces = [c1recv[b, k] for k in range(KVH)]
        rows = [c1ml[b, k] for k in range(KVH)]
        for k in range(KVH):
            c3send[b, k] = pick(pieces, slots[k])
            c3sml[b, k] = pick(rows, slots[k])
        c3recv[b, t] = c3send[b, t]
        c3ml[b, t] = c3sml[b, t]
        for d in (4, 5, 3, 2, 6, 7, 1):
            tt = (t + d) % 8
            send(c3send.at[b, tt], c3recv.at[b, t], ssem.at[C3, b], rsem.at[C3, b], {"tp": tt})
            send(c3sml.at[b, tt], c3ml.at[b, t], ssem.at[C3M, b], rsem.at[C3M, b], {"tp": tt})

    def c4(b):
        got(c3recv.at[b, pl.ds(0, 7)], rsem.at[C3, b])
        got(c3ml.at[b, pl.ds(0, 7)], rsem.at[C3M, b])
        ml = c3ml[b].reshape(8, HD)
        top = jnp.max(ml, axis=0, keepdims=True)
        scale = jnp.exp2((ml - top) * EXP2_SCALE)
        total = jnp.sum(ml * pltpu.roll(scale, QT, 1), axis=0, keepdims=True)
        scale = scale / pltpu.roll(jnp.broadcast_to(total, (8, HD)), QT, 1)
        x = c3recv[b, 0].astype(F32) * to_rows(scale[:1])
        for k in range(1, 8):
            x = x + c3recv[b, k].astype(F32) * to_rows(scale[k : k + 1])
        attall[b, s] = x.astype(BF16)
        for d in (6, 2, 3, 5, 7, 1, 4):
            piece = attall.at[b, s]
            send(piece, piece, ssem.at[C4, b], rsem.at[C4, b], {"seq": (s + d) % 8})

    def c5(b):
        got(c1recv.at[b, pl.ds(0, 7)], rsem.at[C4, b])
        x = jnp.concatenate([attall[b, j] for j in range(GS)], axis=1)
        y = jnp.dot(x, w[...], preferred_element_type=F32)

        k, core = divmod(sequence(b), 2)

        @pl.when(c == core)
        def _():
            yown[k] = y

        @pl.when(c != core)
        def _():
            ysend[k] = y.astype(BF16)
            send(ysend.at[k], d1recv.at[k], dssem.at[0, k], drsem.at[0, k], partner)

    def d2(b):
        k, core = divmod(sequence(b), 2)

        @pl.when(c == core)
        def _():
            got(d1recv.at[k], drsem.at[0, k])
            d2send[k] = (yown[k] + d1recv[k].astype(F32)).astype(BF16)

            @pl.when(z == k)
            def _():
                d2recv[k] = d2send[k]

            @pl.when(z != k)
            def _():
                send(d2send.at[k], d2recv.at[z], dssem.at[1, k], drsem.at[1, 0], {"tp": sequence(b)})

    q0(0)
    q1(0)
    for b in range(1, 4):
        q0(b)
    q1(1)
    q1(2)
    for b in range(4, NB):
        q0(b)
    q1(3)
    q2(0)
    q2(1)
    q1(4)
    q2(2)
    q1(5)
    q3(0)
    kv_load(0).wait()
    qk(0, 0)

    def guarded(step, b):
        pl.when((b >= 0) & (b < NB))(lambda: step(b))

    def steps_at(b):
        for step, lead in ((q4, 0), (c1, -1), (q3, 1), (q2, 3), (q1, 6), (c3, -4), (c4, -7)):
            if not isinstance(b, int):
                if step is not c4:
                    guarded(step, b + lead)
            elif 0 <= b + lead < NB:
                step(b + lead)

    def body(b, carry):
        steps_at(b)
        kv_load(b + 1).wait()
        qk(b, 1)
        weigh(0)
        pv(b, 0)
        weigh(1)
        qk(b + 1, 0)
        pv(b, 1)
        return carry

    lax.fori_loop(0, NB - 1, body, 0)
    last = NB - 1
    steps_at(last)
    qk(last, 1)
    weigh(0)
    pv(last, 0)
    weigh(1)
    pv(last, 1)
    c1(last)
    wload.wait()
    for step, b in (
        (c3, 4), (c3, 5), (c4, 1), (c4, 2), (c3, 6), (c4, 3), (c3, 7), (c5, 0), (c4, 4), (c5, 1), (c4, 5), (c5, 2), (c4, 6), (d2, 0), (c5, 3), (d2, 1), (c4, 7), (c5, 4), (d2, 2), (c5, 5), (d2, 3), (c5, 6), (d2, 4), (d2, 5), (c5, 7), (d2, 6), (d2, 7),
    ):
        step(b)
    got(d2recv.at[pl.ds(0, 3)], drsem.at[1, 0])
    out_ref[0] = jnp.sum(d2recv[...].astype(F32), axis=0).astype(BF16)

    def drain(b, carry):
        sent(q0recv.at[b], ssem.at[Q0, b])
        sent(q1recv.at[b, pl.ds(0, 3)], ssem.at[Q1, b])
        sent(q1recv.at[b, pl.ds(0, 3)], ssem.at[Q2, b])
        sent(qall.at[b, pl.ds(0, 4)], ssem.at[Q3, b])
        for k in (C1, C3, C4):
            sent(c1recv.at[b, pl.ds(0, 7)], ssem.at[k, b])
        for k in (C1M, C3M):
            sent(c1ml.at[b, pl.ds(0, 7)], ssem.at[k, b])
        return carry

    lax.fori_loop(0, NB, drain, 0)
    for k in range(4):
        sent(d1recv.at[k], dssem.at[0, k])
        pl.when(z != k)(lambda k=k: sent(d2send.at[k], dssem.at[1, k]))


def local(query, cache, head_of_slot, lengths, out_weight):
    length = cache.shape[1]
    entries = cache.reshape(NB, length, 2 * HD)
    wide = out_weight.shape[1]
    vm = pltpu.VMEM
    dma = pltpu.SemaphoreType.DMA
    anywhere = pl.BlockSpec(memory_space=pl.ANY)
    return pl.pallas_call(
        kernel,
        out_shape=jax.ShapeDtypeStruct((1, QT, wide), BF16),
        in_specs=[anywhere] * 5,
        out_specs=pl.BlockSpec(memory_space=pltpu.VMEM),
        scratch_shapes=[
            pltpu.SMEM((KVH,), jnp.int32),
            pltpu.SMEM((NB,), jnp.int32),
            vm((NB, QT, GS * HD), BF16),
            vm((NB, QT, 4 * HD), BF16),
            vm((NB, 4, QT, HD), BF16),
            vm((NB, 4, QT, HD), BF16),
            vm((NB, GS, QT, HD), BF16),
            vm((NB, length, 2 * HD), BF16),
            vm(out_weight.shape, BF16),
            vm((TILE, length), F32),
            vm((TILE, length), F32),
            vm((TILE, length), BF16),
            vm((TILE, length), BF16),
            vm((TILE, HD), F32),
            vm((TILE, HD), F32),
            vm((NB, GS, QT, HD), BF16),
            vm((NB, GS, 1, HD), F32),
            vm((NB, KVH, QT, HD), BF16),
            vm((NB, KVH, 1, HD), F32),
            vm((NB, KVH, QT, HD), BF16),
            vm((NB, KVH, 1, HD), F32),
            vm((NB, 8, QT, HD), BF16),
            vm((NB, 8, 1, HD), F32),
            vm((NB, GS, QT, HD), BF16),
            vm((4, QT, wide), BF16),
            vm((4, QT, wide), F32),
            vm((4, QT, wide), BF16),
            vm((4, QT, wide), BF16),
            vm((4, QT, wide), BF16),
            dma((9, NB)),
            dma((9, NB)),
            dma((2, 4)),
            dma((2, 4)),
            dma((2 * NB + 4,)),
        ],
        compiler_params=pltpu.CompilerParams(
            collective_id=0, has_side_effects=True, vmem_limit_bytes=40 * 2**20
        ),
        name="attend",
    )(*[pltpu.with_memory_space_constraint(x, pltpu.HBM) for x in (head_of_slot, lengths, query, entries, out_weight)])


def solution(mesh):
    in_specs = (
        P("grp", None, "tp"),
        P("grp", "tp", "seq", None),
        P("grp"),
        P("grp"),
        P("tp", "seq"),
    )
    out_specs = P(("grp", "tp"), None, "seq")
    return jax.shard_map(local, mesh=mesh, in_specs=in_specs, out_specs=out_specs, check_vma=False)
```
